512 devices in a mesh: op: 32 (over x, y_hi, core), sec: 16 (over z, y_lo).
Axes of the slice: x: 4, y: 8 (y_hi: 4, y_lo: 2; y = y_hi * 2 + y_lo), z: 8, core: 2. Of those that a mesh axis runs over, the one named last changes fastest.
Arguments:
- psi: bfloat16 [32, 512, 512], P('sec', 'op'), may hold values from -6 to 6
- left_ops: bfloat16 [64, 32, 512, 512], P('op', 'sec'), may hold values from -0.25 to 0.25
- right_ops: bfloat16 [64, 32, 512, 512], P('op', 'sec'), may hold values from -0.03125 to 0.03125
- conn: int32 [64, 32], P('op', 'sec'), may hold values from 0 to 31, as said below
- dims: int32 [32], P('sec'), may hold values from 128 to 512
Outputs:
- sigma: bfloat16 [32, 512, 512], P('sec', 'op')
The draws below stay inside these ranges and needn't reach their ends.
Inputs may be any that keep to these rules, and one draw needn't show every extreme that they name: conn[k, s] lies in the same group of 2 consecutive sectors as s or in the next group, cyclically over the 32 sectors; both occur.
All inputs are finite; a program needn't handle non-finite values.
Results may differ from the reference program's by a relative error of at most 0.0049.
Values may be sent and summed in bfloat16 or wider, within the bound.
No kernel may reach another device: no remote copies, remote signals or barrier semaphores. Data moves between devices by JAX's collectives and lax.ppermute only.
A program may use at most 64 MiB of HBM per device.

```python
import jax
import jax.numpy as jnp
from jax import lax

B = 512
K_DEV = 2
S_DEV = 2
K = 64
S = 32
N_OP = 32
N_SEC = 16


def draw_conn(key, part):
    first = jax.random.fold_in(key, 11)
    second = jax.random.fold_in(key, 23)
    count = K_DEV * N_OP
    total = S_DEV * N_SEC
    group = jnp.arange(total, dtype=jnp.int32) // S_DEV
    hop = jax.random.randint(first, (count, total), 0, 2, dtype=jnp.int32)
    slot = jax.random.randint(second, (count, total), 0, S_DEV, dtype=jnp.int32)
    return (group[None, :] + hop) % N_SEC * S_DEV + slot


def with_ends(array, key, low, high):
    shape = array.shape
    place = [jax.random.randint(jax.random.fold_in(key, axis), (), 0, shape[axis]) for axis in range(len(shape))]
    array = array.at[tuple(place)].set(low)
    longest = shape.index(max(shape))
    place[longest] = (place[longest] + 1) % shape[longest]
    return array.at[tuple(place)].set(high)


def steps_of(own_key, shape, shards, least, high):
    def one(dim, shards_of):
        heights = jax.random.uniform(jax.random.fold_in(jax.random.fold_in(own_key, 6), dim), (shards_of,), jnp.float32, least / len(shards), high / len(shards))
        return jnp.repeat(jnp.exp(heights), shape[dim] // shards_of).reshape((-1,) + (1,) * (len(shape) - dim - 1))

    level = one(*shards[0])
    for cut in shards[1:]:
        level = level * one(*cut)
    return level


def gaussian(rng, shape, scale, bound, split=(), kind=jnp.bfloat16):
    entries = jax.random.normal(rng, shape, jnp.float32) * scale
    if len(split) > 0:
        entries = steps_of(rng, shape, split, -0.22, 0.18) * entries
    return jnp.clip(entries, min=-bound, max=bound).astype(kind)


def setup_inputs(seed: int = 0) -> dict:
    arg_keys = jax.random.split(jax.random.key(seed), 6)
    return {
        "psi": gaussian(arg_keys[0], (S, B, B), 1.0, 6.0, ((0, 16), (1, 32))),
        "left_ops": gaussian(arg_keys[1], (K, S, B, B), B ** -0.5, 0.25, ((0, 32), (1, 16))),
        "right_ops": gaussian(arg_keys[2], (K, S, B, B), (B * K_DEV * N_OP) ** -0.5, 0.03125, ((0, 32), (1, 16))),
        "conn": draw_conn(jax.random.fold_in(arg_keys[5], 71), 0),
        "dims": with_ends(jax.random.randint(arg_keys[4], (S,), B // 4, B + 1), jax.random.fold_in(arg_keys[4], 1), B // 4, B).astype(jnp.int32),
    }


def block_mask(dims):
    idx = jnp.arange(B, dtype=jnp.int32)
    keep = (idx[None, :, None] < dims[:, None, None]) & (idx[None, None, :] < dims[:, None, None])
    return keep


def reference(psi, left_ops, right_ops, conn, dims):
    masked = jnp.where(block_mask(dims), psi, jnp.zeros_like(psi))
    targets = jnp.arange(S, dtype=jnp.int32)

    def step(total, items):
        left_s, right_s, psi_s, conn_s = items
        half = jnp.einsum("kij,jm->kim", left_s.astype(jnp.float32), psi_s.astype(jnp.float32), precision=lax.Precision.HIGHEST)
        half = half.astype(jnp.bfloat16)
        term = jnp.einsum("kim,knm->kin", half.astype(jnp.float32), right_s.astype(jnp.float32), precision=lax.Precision.HIGHEST)
        onehot = (conn_s[:, None] == targets[None, :]).astype(jnp.float32)
        total = total + jnp.einsum("kt,kin->tin", onehot, term, precision=lax.Precision.HIGHEST)
        return total, None

    items = (jnp.moveaxis(left_ops, 1, 0), jnp.moveaxis(right_ops, 1, 0), masked, jnp.moveaxis(conn, 1, 0))
    total, _ = lax.scan(step, jnp.zeros((S, B, B), jnp.float32), items)
    total = jnp.where(block_mask(dims), total, jnp.zeros_like(total))
    return total.astype(jnp.bfloat16)
```

```python
import jax
import jax.numpy as jnp
from jax import lax
from jax.experimental import pallas as pl
from jax.experimental.pallas import tpu as pltpu
from jax.sharding import Mesh
from jax.sharding import PartitionSpec as P

OP = ("x", "y", "c")
F32 = jnp.float32
BF16 = jnp.bfloat16


def exchanged(x, axis):
    return lax.all_to_all(x, axis, split_axis=0, concat_axis=0, tiled=True)


def shared(x, axis):
    return exchanged(jnp.broadcast_to(x[None], (lax.axis_size(axis),) + x.shape), axis)


def from_partner(x):
    return lax.ppermute(x, "c", [(0, 1), (1, 0)])


def from_behind(x):
    n = lax.axis_size("sec")
    return lax.ppermute(x, "sec", [(i, (i + 1) % n) for i in range(n)])


def in_vmem(x):
    return pltpu.with_memory_space_constraint(x, pltpu.VMEM)


def sums_kernel(where_ref, conn_ref, conn2_ref, dims_ref, near_ref, far_ref, left_ref, right_ref, left2_ref, right2_ref, out_ref, psi_ref, rows_ref, half_ref, term_ref, rights_ref, sems):
    kdev, sdev, width, _ = right_ref.shape
    chips, _, tall, _ = near_ref.shape
    group = where_ref[0]
    core = where_ref[1]
    many = chips * tall
    fetches = []
    for whose in range(2):
        for s in range(sdev):
            group_of = []
            for k in range(kdev):
                right = (right_ref, right2_ref)[whose].at[k, s]
                group_of.append(pltpu.make_async_copy(right, rights_ref.at[whose, k, s], sems.at[whose, s, k]))
                if whose == 1:
                    rows = rows_ref.at[s, kdev + k]
                    group_of.append(pltpu.make_async_copy(left2_ref.at[k, s, :, core], rows, sems.at[2, s, k]))
            fetches.append(group_of)
    for group_of in fetches:
        for fetch in group_of:
            fetch.start()
    cols = lax.broadcasted_iota(jnp.int32, (tall, width), 1)
    row = lax.broadcasted_iota(jnp.int32, (tall, width), 0)
    for s in range(sdev):
        size = dims_ref[s]
        inside = cols < size
        for chip in range(chips):
            for ref, seat in ((near_ref, core), (far_ref, 1 - core)):
                start = pl.multiple_of((chip * 2 + seat) * tall, tall)
                kept = jnp.where(inside & (row + start < size), ref[chip, s].astype(F32), 0.0)
                psi_ref[s, pl.ds(start, tall), :] = kept.astype(BF16)
            for k in range(kdev):
                rows_ref[s, k, chip] = left_ref[k, s, chip, core]
    shares = [None] * (2 * kdev * sdev)
    for whose in range(2):
        conns = (conn_ref, conn2_ref)[whose]
        for s in range(sdev):
            for fetch in fetches[whose * sdev + s]:
                fetch.wait()
            left = rows_ref[s, whose * kdev : (whose + 1) * kdev].reshape(kdev * many, width)
            half_ref[...] = jnp.dot(left, psi_ref[s], preferred_element_type=F32).astype(BF16)
            for k in range(kdev):
                n = (whose * sdev + s) * kdev + k
                term_ref[n] = lax.dot_general(
                    half_ref[k * many : (k + 1) * many, :],
                    rights_ref[whose, k, s],
                    (((1,), (1,)), ((), ())),
                    preferred_element_type=F32,
                )
                target = conns[k, s]
                place = target % sdev + jnp.where(target // sdev != group, sdev, 0)
                shares[n] = [jnp.where(place == t, 1.0, 0.0).astype(F32) for t in range(2 * sdev)]
    wide = width // 2
    for chip in range(chips):
        for cut in range(2):
            terms = [term_ref[n, chip * tall : (chip + 1) * tall, cut * wide : (cut + 1) * wide] for n in range(len(shares))]
            for t in range(2 * sdev):
                total = shares[0][t] * terms[0]
                for n in range(1, len(shares)):
                    total = total + shares[n][t] * terms[n]
                out_ref[chip, t, :, cut * wide : (cut + 1) * wide] = total.astype(BF16)


def slot_sums(where, conn, conn2, dims, near, far, left, right, left2, right2):
    kdev, sdev, width, _ = left.shape
    chips, _, tall, _ = near.shape
    smem = pl.BlockSpec(memory_space=pltpu.SMEM)
    vmem = pl.BlockSpec(memory_space=pltpu.VMEM)
    hbm = pl.BlockSpec(memory_space=pltpu.HBM)
    many = chips * tall
    by_row = (kdev, sdev, chips, 2, tall, width)
    return pl.pallas_call(
        sums_kernel,
        in_specs=[smem] * 4 + [vmem] * 3 + [hbm] * 3,
        out_specs=vmem,
        out_shape=pltpu.VMEM((chips, 2 * sdev, tall, width), BF16),
        scratch_shapes=[
            pltpu.VMEM((sdev, width, width), BF16),
            pltpu.VMEM((sdev, 2 * kdev, chips, tall, width), BF16),
            pltpu.VMEM((kdev * many, width), BF16),
            pltpu.VMEM((2 * kdev * sdev, many, width), F32),
            pltpu.VMEM((2, kdev, sdev, width, width), BF16),
            pltpu.SemaphoreType.DMA((3, sdev, kdev)),
        ],
        compiler_params=pltpu.CompilerParams(vmem_limit_bytes=24 * 2**20),
        name="slot_sums",
    )(where, conn, conn2, dims, *(in_vmem(x) for x in (near, far, left.reshape(by_row))), right, left2.reshape(by_row), right2)


def row_mask(dims, row_start, rows, width):
    row_ids = row_start + jnp.arange(rows, dtype=jnp.int32)
    col_ids = jnp.arange(width, dtype=jnp.int32)
    return (row_ids[None, :, None] < dims[:, None, None]) & (
        col_ids[None, None, :] < dims[:, None, None]
    )


def sigma_rows(psi, left_ops, right_ops, conn, dims):
    sdev, tall, width = psi.shape
    nx, ny = lax.axis_size("x"), lax.axis_size("y")
    left2 = from_partner(left_ops)
    right2 = from_partner(right_ops)
    conn2 = from_partner(conn)
    by_y = shared(psi, "y").reshape(ny, sdev, tall, width)
    by_x = shared(by_y, "x").reshape(nx * ny, sdev, tall, width)
    other = from_partner(by_x)
    where = jnp.stack([lax.axis_index("sec"), lax.axis_index("c")]).astype(jnp.int32)
    both = slot_sums(where, conn, conn2, dims, by_x, other, left_ops, right_ops, left2, right2)
    both = exchanged(both, "x").reshape(nx, ny, 2 * sdev, tall, width)
    both = both.astype(F32).sum(axis=0).astype(BF16)
    both = exchanged(both, "y").astype(F32).sum(axis=0)
    onward = from_behind(both[sdev:].astype(BF16))
    summed = both[:sdev] + onward.astype(F32)
    row_start = lax.axis_index(OP) * tall
    summed = jnp.where(row_mask(dims, row_start, tall, width), summed, jnp.zeros_like(summed))
    return summed.astype(BF16)


def solution(mesh):
    finer = Mesh(mesh.devices.reshape(4, 4, 2, mesh.shape["sec"]), OP + ("sec",))
    in_specs = (
        P("sec", OP, None),
        P(OP, "sec", None, None),
        P(OP, "sec", None, None),
        P(OP, "sec"),
        P("sec"),
    )
    out_specs = P("sec", OP, None)
    return jax.shard_map(sigma_rows, mesh=finer, in_specs=in_specs, out_specs=out_specs, check_vma=False)
```

```python
import jax
import jax.numpy as jnp
from jax import lax
from jax.experimental import pallas as pl
from jax.experimental.pallas import tpu as pltpu
from jax.sharding import Mesh
from jax.sharding import PartitionSpec as P

OP = ("x", "y", "c")
F32 = jnp.float32
BF16 = jnp.bfloat16


def exchanged(x, axis):
    return lax.all_to_all(x, axis, split_axis=0, concat_axis=0, tiled=True)


def shared(x, axis):
    return exchanged(jnp.broadcast_to(x[None], (lax.axis_size(axis),) + x.shape), axis)


def from_partner(x):
    return lax.ppermute(x, "c", [(0, 1), (1, 0)])


def from_behind(x):
    n = lax.axis_size("sec")
    return lax.ppermute(x, "sec", [(i, (i + 1) % n) for i in range(n)])


def in_vmem(x):
    return pltpu.with_memory_space_constraint(x, pltpu.VMEM)


def in_hbm(x):
    return pltpu.with_memory_space_constraint(x, pltpu.HBM)


def sums_kernel(where_ref, conn_ref, conn2_ref, dims_ref, near_ref, far_ref, left_ref, right_ref, left2_ref, right2_ref, own_ref, onward_ref, psi_ref, rows_ref, half_ref, term_ref, rights_ref, sems):
    kdev, sdev, width, _ = right_ref.shape
    chips, _, tall, _ = near_ref.shape
    group = where_ref[0]
    core = where_ref[1]
    many = chips * tall
    fetches = []
    for whose in range(2):
        for s in range(sdev):
            group_of = []
            for k in range(kdev):
                right = (right_ref, right2_ref)[whose].at[k, s]
                group_of.append(pltpu.make_async_copy(right, rights_ref.at[whose, k, s], sems.at[whose, s, k]))
                if whose == 1:
                    rows = rows_ref.at[s, kdev + k]
                    group_of.append(pltpu.make_async_copy(left2_ref.at[k, s, :, core], rows, sems.at[2, s, k]))
            fetches.append(group_of)
    for group_of in fetches:
        for fetch in group_of:
            fetch.start()
    cols = lax.broadcasted_iota(jnp.int32, (tall, width), 1)
    row = lax.broadcasted_iota(jnp.int32, (tall, width), 0)
    for s in range(sdev):
        size = dims_ref[s]
        inside = cols < size
        for chip in range(chips):
            for ref, seat in ((near_ref, core), (far_ref, 1 - core)):
                start = pl.multiple_of((chip * 2 + seat) * tall, tall)
                kept = jnp.where(inside & (row + start < size), ref[chip, s].astype(F32), 0.0)
                psi_ref[s, pl.ds(start, tall), :] = kept.astype(BF16)
            for k in range(kdev):
                rows_ref[s, k, chip] = left_ref[k, s, chip, core]
    shares = [None] * (2 * kdev * sdev)
    for whose in range(2):
        conns = (conn_ref, conn2_ref)[whose]
        for s in range(sdev):
            for fetch in fetches[whose * sdev + s]:
                fetch.wait()
            left = rows_ref[s, whose * kdev : (whose + 1) * kdev].reshape(kdev * many, width)
            half_ref[...] = jnp.dot(left, psi_ref[s], preferred_element_type=F32).astype(BF16)
            for k in range(kdev):
                n = (whose * sdev + s) * kdev + k
                term_ref[n] = lax.dot_general(
                    half_ref[k * many : (k + 1) * many, :],
                    rights_ref[whose, k, s],
                    (((1,), (1,)), ((), ())),
                    preferred_element_type=F32,
                )
                target = conns[k, s]
                place = target % sdev + jnp.where(target // sdev != group, sdev, 0)
                shares[n] = [jnp.where(place == t, 1.0, 0.0).astype(F32) for t in range(2 * sdev)]
    wide = width // 2
    for chip in range(chips):
        for cut in range(2):
            terms = [term_ref[n, chip * tall : (chip + 1) * tall, cut * wide : (cut + 1) * wide] for n in range(len(shares))]
            for t in range(2 * sdev):
                total = shares[0][t] * terms[0]
                for n in range(1, len(shares)):
                    total = total + shares[n][t] * terms[n]
                out_ref = (own_ref, onward_ref)[t // sdev]
                out_ref[chip, t % sdev, :, cut * wide : (cut + 1) * wide] = total.astype(BF16)


def slot_sums(where, conn, conn2, dims, near, far, left, right, left2, right2):
    kdev, sdev, width, _ = left.shape
    chips, _, tall, _ = near.shape
    smem = pl.BlockSpec(memory_space=pltpu.SMEM)
    vmem = pl.BlockSpec(memory_space=pltpu.VMEM)
    hbm = pl.BlockSpec(memory_space=pltpu.HBM)
    many = chips * tall
    by_row = (kdev, sdev, chips, 2, tall, width)
    return pl.pallas_call(
        sums_kernel,
        in_specs=[smem] * 4 + [vmem] * 3 + [hbm] * 3,
        out_specs=[vmem] * 2,
        out_shape=[pltpu.VMEM((chips, sdev, tall, width), BF16)] * 2,
        scratch_shapes=[
            pltpu.VMEM((sdev, width, width), BF16),
            pltpu.VMEM((sdev, 2 * kdev, chips, tall, width), BF16),
            pltpu.VMEM((kdev * many, width), BF16),
            pltpu.VMEM((2 * kdev * sdev, many, width), F32),
            pltpu.VMEM((2, kdev, sdev, width, width), BF16),
            pltpu.SemaphoreType.DMA((3, sdev, kdev)),
        ],
        compiler_params=pltpu.CompilerParams(vmem_limit_bytes=24 * 2**20),
        name="slot_sums",
    )(where, conn, conn2, dims, *(in_vmem(x) for x in (near, far, left.reshape(by_row))), *(in_hbm(x) for x in (right, left2.reshape(by_row), right2)))


def row_mask(dims, row_start, rows, width):
    row_ids = row_start + jnp.arange(rows, dtype=jnp.int32)
    col_ids = jnp.arange(width, dtype=jnp.int32)
    return (row_ids[None, :, None] < dims[:, None, None]) & (
        col_ids[None, None, :] < dims[:, None, None]
    )


def sigma_rows(psi, left_ops, right_ops, conn, dims):
    sdev, tall, width = psi.shape
    nx, ny = lax.axis_size("x"), lax.axis_size("y")
    left2 = from_partner(left_ops)
    right2 = from_partner(right_ops)
    conn2 = from_partner(conn)
    by_y = shared(psi, "y").reshape(ny, sdev, tall, width)
    by_x = shared(by_y, "x").reshape(nx * ny, sdev, tall, width)
    other = from_partner(by_x)
    where = jnp.stack([lax.axis_index("sec"), lax.axis_index("c")]).astype(jnp.int32)
    own, onward = slot_sums(where, conn, conn2, dims, by_x, other, left_ops, right_ops, left2, right2)
    by_chip = (nx, ny, sdev, tall, width)
    onward = exchanged(onward, "x").reshape(by_chip).astype(F32).sum(axis=0).astype(BF16)
    own = exchanged(own, "x").reshape(by_chip).astype(F32).sum(axis=0)
    onward = from_behind(onward)
    summed = exchanged((own + onward.astype(F32)).astype(BF16), "y").astype(F32).sum(axis=0)
    row_start = lax.axis_index(OP) * tall
    summed = jnp.where(row_mask(dims, row_start, tall, width), summed, jnp.zeros_like(summed))
    return summed.astype(BF16)


def solution(mesh):
    finer = Mesh(mesh.devices.reshape(4, 4, 2, mesh.shape["sec"]), OP + ("sec",))
    in_specs = (
        P("sec", OP, None),
        P(OP, "sec", None, None),
        P(OP, "sec", None, None),
        P(OP, "sec"),
        P("sec"),
    )
    out_specs = P("sec", OP, None)
    return jax.shard_map(sigma_rows, mesh=finer, in_specs=in_specs, out_specs=out_specs, check_vma=False)
```

```python
import jax
import jax.numpy as jnp
from jax import lax
from jax.experimental import pallas as pl
from jax.experimental.pallas import tpu as pltpu
from jax.sharding import Mesh
from jax.sharding import PartitionSpec as P

OP = ("x", "y", "c")
F32 = jnp.float32
BF16 = jnp.bfloat16


def exchanged(x, axis):
    return lax.all_to_all(x, axis, split_axis=0, concat_axis=0, tiled=True)


def shared(x, axis):
    return exchanged(jnp.broadcast_to(x[None], (lax.axis_size(axis),) + x.shape), axis)


def from_partner(x):
    return lax.ppermute(x, "c", [(0, 1), (1, 0)])


def from_behind(x):
    n = lax.axis_size("sec")
    return lax.ppermute(x, "sec", [(i, (i + 1) % n) for i in range(n)])


def in_vmem(x):
    return pltpu.with_memory_space_constraint(x, pltpu.VMEM)


def in_hbm(x):
    return pltpu.with_memory_space_constraint(x, pltpu.HBM)


def fetch_kernel(where_ref, left_ref, right_ref, rows_ref, rights_ref, sems):
    core = where_ref[1]
    fetches = []
    for k in range(right_ref.shape[0]):
        fetches.append(pltpu.make_async_copy(left_ref.at[k, 0, :, core], rows_ref.at[k], sems.at[0, k]))
        fetches.append(pltpu.make_async_copy(right_ref.at[k, 0], rights_ref.at[k], sems.at[1, k]))
    for fetch in fetches:
        fetch.start()
    for fetch in fetches:
        fetch.wait()


def fetched(where, left, right):
    kdev, _, chips, _, tall, width = left.shape
    hbm = pl.BlockSpec(memory_space=pltpu.HBM)
    return pl.pallas_call(
        fetch_kernel,
        in_specs=[pl.BlockSpec(memory_space=pltpu.SMEM), hbm, hbm],
        out_specs=[pl.BlockSpec(memory_space=pltpu.VMEM)] * 2,
        out_shape=[
            pltpu.VMEM((kdev, chips, tall, width), BF16),
            pltpu.VMEM((kdev, width, width), BF16),
        ],
        scratch_shapes=[pltpu.SemaphoreType.DMA((2, kdev))],
        compiler_params=pltpu.CompilerParams(vmem_limit_bytes=2**20),
        name="fetch",
    )(where, in_hbm(left), in_hbm(right))


def sums_kernel(where_ref, conn_ref, conn2_ref, dims_ref, near_ref, far_ref, rows0_ref, right0_ref, left_ref, right_ref, left2_ref, right2_ref, own_ref, onward_ref, psi_ref, rows_ref, rights_ref, half_ref, sum_ref, sems):
    kdev, sdev, width, _ = right_ref.shape
    chips, _, tall, _ = near_ref.shape
    group = where_ref[0]
    core = where_ref[1]
    many = chips * tall
    steps = [(0, 0, rows0_ref, right0_ref, ())]
    for whose, s in ((0, 1), (1, 0), (1, 1)):
        n = len(steps) - 1
        left, right = ((left_ref, right_ref), (left2_ref, right2_ref))[whose]
        fetches = []
        for k in range(kdev):
            fetches.append(pltpu.make_async_copy(left.at[k, s, :, core], rows_ref.at[n, k], sems.at[0, n, k]))
            fetches.append(pltpu.make_async_copy(right.at[k, s], rights_ref.at[n, k], sems.at[1, n, k]))
        for fetch in fetches:
            fetch.start()
        steps.append((whose, s, rows_ref.at[n], rights_ref.at[n], fetches))
    cols = lax.broadcasted_iota(jnp.int32, (tall, width), 1)
    row = lax.broadcasted_iota(jnp.int32, (tall, width), 0)
    for s in range(sdev):
        size = dims_ref[s]
        inside = cols < size
        for chip in range(chips):
            for ref, seat in ((near_ref, core), (far_ref, 1 - core)):
                start = pl.multiple_of((chip * 2 + seat) * tall, tall)
                kept = jnp.where(inside & (row + start < size), ref[chip, s].astype(F32), 0.0)
                psi_ref[s, pl.ds(start, tall), :] = kept.astype(BF16)
    sum_ref[...] = jnp.zeros_like(sum_ref)
    for whose, s, rows, rights, fetches in steps:
        for fetch in fetches:
            fetch.wait()
        left = rows[...].reshape(kdev * many, width)
        half_ref[...] = jnp.dot(left, psi_ref[s], preferred_element_type=F32).astype(BF16)
        for k in range(kdev):
            target = (conn_ref, conn2_ref)[whose][k, s]
            place = target % sdev + jnp.where(target // sdev != group, sdev, 0)
            sum_ref[place] += lax.dot_general(
                half_ref[k * many : (k + 1) * many, :],
                rights[k],
                (((1,), (1,)), ((), ())),
                preferred_element_type=F32,
            )
    for t in range(2 * sdev):
        out_ref = (own_ref, onward_ref)[t // sdev]
        for chip in range(chips):
            out_ref[chip, t % sdev] = sum_ref[t, chip * tall : (chip + 1) * tall, :].astype(BF16)


def slot_sums(where, conn, conn2, dims, near, far, rows0, right0, left, right, left2, right2):
    kdev, sdev, chips, _, tall, width = left.shape
    assert sdev == 2
    rest = 2 * sdev - 1
    smem = pl.BlockSpec(memory_space=pltpu.SMEM)
    vmem = pl.BlockSpec(memory_space=pltpu.VMEM)
    hbm = pl.BlockSpec(memory_space=pltpu.HBM)
    many = chips * tall
    return pl.pallas_call(
        sums_kernel,
        in_specs=[smem] * 4 + [vmem] * 4 + [hbm] * 4,
        out_specs=[vmem] * 2,
        out_shape=[pltpu.VMEM((chips, sdev, tall, width), BF16)] * 2,
        scratch_shapes=[
            pltpu.VMEM((sdev, width, width), BF16),
            pltpu.VMEM((rest, kdev, chips, tall, width), BF16),
            pltpu.VMEM((rest, kdev, width, width), BF16),
            pltpu.VMEM((kdev * many, width), BF16),
            pltpu.VMEM((2 * sdev, many, width), F32),
            pltpu.SemaphoreType.DMA((2, rest, kdev)),
        ],
        compiler_params=pltpu.CompilerParams(vmem_limit_bytes=24 * 2**20),
        name="slot_sums",
    )(where, conn, conn2, dims, *(in_vmem(x) for x in (near, far, rows0, right0)), *(in_hbm(x) for x in (left, right, left2, right2)))


def last_kernel(where_ref, dims_ref, parts_ref, out_ref):
    count, sdev, tall, width = parts_ref.shape
    cols = lax.broadcasted_iota(jnp.int32, (tall, width), 1)
    row = lax.broadcasted_iota(jnp.int32, (tall, width), 0) + where_ref[2]
    for s in range(sdev):
        total = parts_ref[0, s].astype(F32)
        for part in range(1, count):
            total = total + parts_ref[part, s].astype(F32)
        size = dims_ref[s]
        out_ref[s] = jnp.where((cols < size) & (row < size), total, 0.0).astype(BF16)


def last_sum(where, dims, parts):
    smem = pl.BlockSpec(memory_space=pltpu.SMEM)
    vmem = pl.BlockSpec(memory_space=pltpu.VMEM)
    return pl.pallas_call(
        last_kernel,
        in_specs=[smem, smem, vmem],
        out_specs=vmem,
        out_shape=jax.ShapeDtypeStruct(parts.shape[1:], BF16),
        compiler_params=pltpu.CompilerParams(vmem_limit_bytes=4 * 2**20),
        name="last_sum",
    )(where, dims, in_vmem(parts))


def sigma_rows(psi, left_ops, right_ops, conn, dims):
    sdev, tall, width = psi.shape
    nx, ny = lax.axis_size("x"), lax.axis_size("y")
    places = (lax.axis_index("sec"), lax.axis_index("c"), lax.axis_index(OP) * tall)
    where = jnp.stack(places).astype(jnp.int32)
    by_row = left_ops.shape[:2] + (nx * ny, 2, tall, width)
    left2 = from_partner(left_ops).reshape(by_row)
    right2 = from_partner(right_ops)
    conn2 = from_partner(conn)
    left = left_ops.reshape(by_row)
    rows0, right0 = fetched(where, left, right_ops)
    by_y = shared(psi, "y").reshape(ny, sdev, tall, width)
    by_x = shared(by_y, "x").reshape(nx * ny, sdev, tall, width)
    other = from_partner(by_x)
    own, onward = slot_sums(where, conn, conn2, dims, by_x, other, rows0, right0, left, right_ops, left2, right2)
    by_chip = (nx, ny, sdev, tall, width)
    onward = exchanged(onward, "x").reshape(by_chip).astype(F32).sum(axis=0).astype(BF16)
    onward = from_behind(onward)
    own = exchanged(own, "x").reshape(by_chip).astype(F32).sum(axis=0)
    parts = exchanged((own + onward.astype(F32)).astype(BF16), "y")
    return last_sum(where, dims, parts)


def solution(mesh):
    finer = Mesh(mesh.devices.reshape(4, 4, 2, mesh.shape["sec"]), OP + ("sec",))
    in_specs = (
        P("sec", OP, None),
        P(OP, "sec", None, None),
        P(OP, "sec", None, None),
        P(OP, "sec"),
        P("sec"),
    )
    out_specs = P("sec", OP, None)
    return jax.shard_map(sigma_rows, mesh=finer, in_specs=in_specs, out_specs=out_specs, check_vma=False)
```

```python
import jax
import jax.numpy as jnp
from jax import lax
from jax.experimental import pallas as pl
from jax.experimental.pallas import tpu as pltpu
from jax.sharding import Mesh
from jax.sharding import PartitionSpec as P

OP = ("x", "y", "c")
F32 = jnp.float32
BF16 = jnp.bfloat16


def exchanged(x, axis):
    return lax.all_to_all(x, axis, split_axis=0, concat_axis=0, tiled=True)


def shared(x, axis):
    return exchanged(jnp.broadcast_to(x[None], (lax.axis_size(axis),) + x.shape), axis)


def from_partner(x):
    return lax.ppermute(x, "c", [(0, 1), (1, 0)])


def from_behind(x):
    n = lax.axis_size("sec")
    return lax.ppermute(x, "sec", [(i, (i + 1) % n) for i in range(n)])


def in_vmem(x):
    return pltpu.with_memory_space_constraint(x, pltpu.VMEM)


def in_hbm(x):
    return pltpu.with_memory_space_constraint(x, pltpu.HBM)


def fetch_kernel(where_ref, left_ref, right_ref, rows_ref, rights_ref, sems):
    core = where_ref[1]
    fetches = []
    for k in range(right_ref.shape[0]):
        fetches.append(pltpu.make_async_copy(left_ref.at[k, 0, :, core], rows_ref.at[k], sems.at[0, k]))
        fetches.append(pltpu.make_async_copy(right_ref.at[k, 0], rights_ref.at[k], sems.at[1, k]))
    for fetch in fetches:
        fetch.start()
    for fetch in fetches:
        fetch.wait()


def fetched(where, left, right):
    kdev, _, chips, _, tall, width = left.shape
    hbm = pl.BlockSpec(memory_space=pltpu.HBM)
    return pl.pallas_call(
        fetch_kernel,
        in_specs=[pl.BlockSpec(memory_space=pltpu.SMEM), hbm, hbm],
        out_specs=[pl.BlockSpec(memory_space=pltpu.VMEM)] * 2,
        out_shape=[
            pltpu.VMEM((kdev, chips, tall, width), BF16),
            pltpu.VMEM((kdev, width, width), BF16),
        ],
        scratch_shapes=[pltpu.SemaphoreType.DMA((2, kdev))],
        compiler_params=pltpu.CompilerParams(vmem_limit_bytes=2**20),
        name="fetch",
    )(where, in_hbm(left), in_hbm(right))


def sums_kernel(where_ref, conn_ref, conn2_ref, dims_ref, near_ref, far_ref, rows0_ref, right0_ref, left_ref, right_ref, left2_ref, right2_ref, own_ref, onward_ref, psi_ref, rows_ref, rights_ref, half_ref, sum_ref, sems):
    kdev, sdev, width, _ = right_ref.shape
    chips, _, tall, _ = near_ref.shape
    group = where_ref[0]
    core = where_ref[1]
    many = chips * tall
    steps = [(0, 0, rows0_ref, right0_ref, ())]
    for whose, s in ((0, 1), (1, 0), (1, 1)):
        n = len(steps) - 1
        left, right = ((left_ref, right_ref), (left2_ref, right2_ref))[whose]
        fetches = []
        for k in range(kdev):
            fetches.append(pltpu.make_async_copy(left.at[k, s, :, core], rows_ref.at[n, k], sems.at[0, n, k]))
            fetches.append(pltpu.make_async_copy(right.at[k, s], rights_ref.at[n, k], sems.at[1, n, k]))
        steps.append((whose, s, rows_ref.at[n], rights_ref.at[n], fetches))
        for fetch in fetches:
            fetch.start()
    cols = lax.broadcasted_iota(jnp.int32, (tall, width), 1)
    row = lax.broadcasted_iota(jnp.int32, (tall, width), 0)

    @pl.loop(0, chips)
    def _(chip):
        for s in range(sdev):
            size = dims_ref[s]
            for ref, seat in ((near_ref, core), (far_ref, 1 - core)):
                start = pl.multiple_of((chip * 2 + seat) * tall, tall)
                kept = (cols < size) & (row + start < size)
                psi_ref[s, pl.ds(start, tall), :] = jnp.where(kept, ref[chip, s].astype(F32), 0.0).astype(BF16)

    sum_ref[...] = jnp.zeros_like(sum_ref)
    for whose, s, rows, rights, fetches in steps:
        for fetch in fetches:
            fetch.wait()
        left = rows[...].reshape(kdev * many, width)
        half_ref[...] = jnp.dot(left, psi_ref[s], preferred_element_type=F32).astype(BF16)
        for k in range(kdev):
            target = (conn_ref, conn2_ref)[whose][k, s]
            place = target % sdev + jnp.where(target // sdev != group, sdev, 0)
            sum_ref[place] += lax.dot_general(
                half_ref[k * many : (k + 1) * many, :],
                rights[k],
                (((1,), (1,)), ((), ())),
                preferred_element_type=F32,
            )
    for t in range(2 * sdev):
        out_ref = (own_ref, onward_ref)[t // sdev]
        for chip in range(chips):
            out_ref[chip, t % sdev] = sum_ref[t, chip * tall : (chip + 1) * tall, :].astype(BF16)


def slot_sums(where, conn, conn2, dims, near, far, rows0, right0, left, right, left2, right2):
    kdev, sdev, chips, _, tall, width = left.shape
    assert sdev == 2
    rest = 2 * sdev - 1
    smem = pl.BlockSpec(memory_space=pltpu.SMEM)
    vmem = pl.BlockSpec(memory_space=pltpu.VMEM)
    hbm = pl.BlockSpec(memory_space=pltpu.HBM)
    many = chips * tall
    return pl.pallas_call(
        sums_kernel,
        in_specs=[smem] * 4 + [vmem] * 4 + [hbm] * 4,
        out_specs=[vmem] * 2,
        out_shape=[pltpu.VMEM((chips, sdev, tall, width), BF16)] * 2,
        scratch_shapes=[
            pltpu.VMEM((sdev, width, width), BF16),
            pltpu.VMEM((rest, kdev, chips, tall, width), BF16),
            pltpu.VMEM((rest, kdev, width, width), BF16),
            pltpu.VMEM((kdev * many, width), BF16),
            pltpu.VMEM((2 * sdev, many, width), F32),
            pltpu.SemaphoreType.DMA((2, rest, kdev)),
        ],
        compiler_params=pltpu.CompilerParams(vmem_limit_bytes=24 * 2**20),
        name="slot_sums",
    )(where, conn, conn2, dims, *(in_vmem(x) for x in (near, far, rows0, right0)), *(in_hbm(x) for x in (left, right, left2, right2)))


def kept_entries(dims, row_start, rows, width):
    row_ids = row_start + jnp.arange(rows, dtype=jnp.int32)
    col_ids = jnp.arange(width, dtype=jnp.int32)
    return (row_ids[None, :, None] < dims[:, None, None]) & (
        col_ids[None, None, :] < dims[:, None, None]
    )


def sigma_rows(psi, left_ops, right_ops, conn, dims):
    sdev, tall, width = psi.shape
    nx, ny = lax.axis_size("x"), lax.axis_size("y")
    places = (lax.axis_index("sec"), lax.axis_index("c"), lax.axis_index(OP) * tall)
    where = jnp.stack(places).astype(jnp.int32)
    by_row = left_ops.shape[:2] + (nx * ny, 2, tall, width)
    left2 = from_partner(left_ops).reshape(by_row)
    right2 = from_partner(right_ops)
    conn2 = from_partner(conn)
    left = left_ops.reshape(by_row)
    rows0, right0 = fetched(where, left, right_ops)
    by_y = shared(psi, "y").reshape(ny, sdev, tall, width)
    by_x = shared(by_y, "x").reshape(nx * ny, sdev, tall, width)
    kept = kept_entries(dims, places[2], tall, width)
    by_x, kept = lax.optimization_barrier((by_x, kept))
    other = from_partner(by_x)
    own, onward = slot_sums(where, conn, conn2, dims, by_x, other, rows0, right0, left, right_ops, left2, right2)
    by_chip = (nx, ny, sdev, tall, width)
    onward = exchanged(onward, "x").reshape(by_chip).astype(F32).sum(axis=0).astype(BF16)
    onward = from_behind(onward)
    own = exchanged(own, "x").reshape(by_chip).astype(F32).sum(axis=0)
    summed = exchanged((own + onward.astype(F32)).astype(BF16), "y").astype(F32).sum(axis=0)
    return jnp.where(kept, summed, jnp.zeros_like(summed)).astype(BF16)


def solution(mesh):
    finer = Mesh(mesh.devices.reshape(4, 4, 2, mesh.shape["sec"]), OP + ("sec",))
    in_specs = (
        P("sec", OP, None),
        P(OP, "sec", None, None),
        P(OP, "sec", None, None),
        P(OP, "sec"),
        P("sec"),
    )
    out_specs = P("sec", OP, None)
    return jax.shard_map(sigma_rows, mesh=finer, in_specs=in_specs, out_specs=out_specs, check_vma=False)
```

```python
import jax
import jax.numpy as jnp
from jax import lax
from jax.experimental import pallas as pl
from jax.experimental.pallas import tpu as pltpu
from jax.sharding import Mesh
from jax.sharding import PartitionSpec as P

OP = ("x", "y", "c")
F32 = jnp.float32
BF16 = jnp.bfloat16


def exchanged(x, axis):
    return lax.all_to_all(x, axis, split_axis=0, concat_axis=0, tiled=True)


def shared(x, axis):
    return exchanged(jnp.broadcast_to(x[None], (lax.axis_size(axis),) + x.shape), axis)


def from_partner(x):
    return lax.ppermute(x, "c", [(0, 1), (1, 0)])


def from_behind(x):
    n = lax.axis_size("sec")
    return lax.ppermute(x, "sec", [(i, (i + 1) % n) for i in range(n)])


def in_vmem(x):
    return pltpu.with_memory_space_constraint(x, pltpu.VMEM)


def in_hbm(x):
    return pltpu.with_memory_space_constraint(x, pltpu.HBM)


def fetch_kernel(where_ref, left_ref, right_ref, rows_ref, rights_ref, sems):
    kdev, sdev = right_ref.shape[:2]
    core = where_ref[1]
    fetches = []
    for k in range(kdev):
        for s in range(sdev):
            fetches.append(pltpu.make_async_copy(left_ref.at[k, s, :, core], rows_ref.at[s, k], sems.at[s, k]))
        fetches.append(pltpu.make_async_copy(right_ref.at[k, 0], rights_ref.at[k], sems.at[sdev, k]))
    for fetch in fetches:
        fetch.start()
    for fetch in fetches:
        fetch.wait()


def fetched(where, left, right):
    kdev, sdev, chips, _, tall, width = left.shape
    hbm = pl.BlockSpec(memory_space=pltpu.HBM)
    return pl.pallas_call(
        fetch_kernel,
        in_specs=[pl.BlockSpec(memory_space=pltpu.SMEM), hbm, hbm],
        out_specs=[pl.BlockSpec(memory_space=pltpu.VMEM)] * 2,
        out_shape=[
            pltpu.VMEM((sdev, kdev, chips, tall, width), BF16),
            pltpu.VMEM((kdev, width, width), BF16),
        ],
        scratch_shapes=[pltpu.SemaphoreType.DMA((sdev + 1, kdev))],
        compiler_params=pltpu.CompilerParams(vmem_limit_bytes=2**20),
        name="fetch",
    )(where, in_hbm(left), in_hbm(right))


def sums_kernel(where_ref, conn_ref, conn2_ref, dims_ref, near_ref, far_ref, rows0_ref, right0_ref, right_ref, left2_ref, right2_ref, own_ref, onward_ref, psi_ref, rows_ref, rights_ref, half_ref, sum_ref, sems):
    kdev, sdev, width, _ = right_ref.shape
    chips, _, tall, _ = near_ref.shape
    group = where_ref[0]
    core = where_ref[1]
    many = chips * tall
    steps = [(0, 0, rows0_ref.at[0], right0_ref, (), ())]
    for whose, s in ((0, 1), (1, 0), (1, 1)):
        n = len(steps) - 1
        rights = (right_ref, right2_ref)[whose]
        row_copies, right_copies = [], []
        rows = rows0_ref.at[s]
        if whose == 1:
            rows = rows_ref.at[s]
            for k in range(kdev):
                row_copies.append(pltpu.make_async_copy(left2_ref.at[k, s, :, core], rows.at[k], sems.at[0, n, k]))
        for k in range(kdev):
            right_copies.append(pltpu.make_async_copy(rights.at[k, s], rights_ref.at[n, k], sems.at[1, n, k]))
        for fetch in row_copies + right_copies:
            fetch.start()
        steps.append((whose, s, rows, rights_ref.at[n], row_copies, right_copies))
    cols = lax.broadcasted_iota(jnp.int32, (tall, width), 1)
    row = lax.broadcasted_iota(jnp.int32, (tall, width), 0)

    @pl.loop(0, chips)
    def _(chip):
        for s in range(sdev):
            size = dims_ref[s]
            for ref, seat in ((near_ref, core), (far_ref, 1 - core)):
                start = pl.multiple_of((chip * 2 + seat) * tall, tall)
                kept = (cols < size) & (row + start < size)
                psi_ref[s, pl.ds(start, tall), :] = jnp.where(kept, ref[chip, s].astype(F32), 0.0).astype(BF16)

    sum_ref[...] = jnp.zeros_like(sum_ref)
    for whose, s, rows, rights, row_copies, right_copies in steps:
        for fetch in row_copies:
            fetch.wait()
        left = rows[...].reshape(kdev * many, width)
        half_ref[...] = jnp.dot(left, psi_ref[s], preferred_element_type=F32).astype(BF16)
        for k in range(kdev):
            if right_copies:
                right_copies[k].wait()
            target = (conn_ref, conn2_ref)[whose][k, s]
            place = target % sdev + jnp.where(target // sdev != group, sdev, 0)
            sum_ref[place] += lax.dot_general(
                half_ref[k * many : (k + 1) * many, :],
                rights[k],
                (((1,), (1,)), ((), ())),
                preferred_element_type=F32,
            )
    for t in range(2 * sdev):
        out_ref = (own_ref, onward_ref)[t // sdev]
        for chip in range(chips):
            out_ref[chip, t % sdev] = sum_ref[t, chip * tall : (chip + 1) * tall, :].astype(BF16)


def slot_sums(where, conn, conn2, dims, near, far, rows0, right0, right, left2, right2):
    kdev, sdev, chips, _, tall, width = left2.shape
    assert sdev == 2
    rest = 2 * sdev - 1
    smem = pl.BlockSpec(memory_space=pltpu.SMEM)
    vmem = pl.BlockSpec(memory_space=pltpu.VMEM)
    hbm = pl.BlockSpec(memory_space=pltpu.HBM)
    many = chips * tall
    return pl.pallas_call(
        sums_kernel,
        in_specs=[smem] * 4 + [vmem] * 4 + [hbm] * 3,
        out_specs=[vmem] * 2,
        out_shape=[pltpu.VMEM((chips, sdev, tall, width), BF16)] * 2,
        scratch_shapes=[
            pltpu.VMEM((sdev, width, width), BF16),
            pltpu.VMEM((sdev, kdev, chips, tall, width), BF16),
            pltpu.VMEM((rest, kdev, width, width), BF16),
            pltpu.VMEM((kdev * many, width), BF16),
            pltpu.VMEM((2 * sdev, many, width), F32),
            pltpu.SemaphoreType.DMA((2, rest, kdev)),
        ],
        compiler_params=pltpu.CompilerParams(vmem_limit_bytes=24 * 2**20),
        name="slot_sums",
    )(where, conn, conn2, dims, *(in_vmem(x) for x in (near, far, rows0, right0)), *(in_hbm(x) for x in (right, left2, right2)))


def kept_entries(dims, row_start, rows, width):
    row_ids = row_start + jnp.arange(rows, dtype=jnp.int32)
    col_ids = jnp.arange(width, dtype=jnp.int32)
    return (row_ids[None, :, None] < dims[:, None, None]) & (
        col_ids[None, None, :] < dims[:, None, None]
    )


def sigma_rows(psi, left_ops, right_ops, conn, dims):
    sdev, tall, width = psi.shape
    nx, ny = lax.axis_size("x"), lax.axis_size("y")
    places = (lax.axis_index("sec"), lax.axis_index("c"), lax.axis_index(OP) * tall)
    where = jnp.stack(places).astype(jnp.int32)
    by_row = left_ops.shape[:2] + (nx * ny, 2, tall, width)
    left2 = from_partner(left_ops).reshape(by_row)
    right2 = from_partner(right_ops)
    conn2 = from_partner(conn)
    left = left_ops.reshape(by_row)
    rows0, right0 = fetched(where, left, right_ops)
    by_y = shared(psi, "y").reshape(ny, sdev, tall, width)
    kept = kept_entries(dims, places[2], tall, width)
    by_y, kept = lax.optimization_barrier((by_y, kept))
    by_x = shared(by_y, "x").reshape(nx * ny, sdev, tall, width)
    other = from_partner(by_x)
    own, onward = slot_sums(where, conn, conn2, dims, by_x, other, rows0, right0, right_ops, left2, right2)
    by_chip = (nx, ny, sdev, tall, width)
    onward = exchanged(onward, "x").reshape(by_chip).astype(F32).sum(axis=0).astype(BF16)
    onward = from_behind(onward)
    own = exchanged(own, "x").reshape(by_chip).astype(F32).sum(axis=0)
    summed = exchanged((own + onward.astype(F32)).astype(BF16), "y").astype(F32).sum(axis=0)
    return jnp.where(kept, summed, jnp.zeros_like(summed)).astype(BF16)


def solution(mesh):
    finer = Mesh(mesh.devices.reshape(4, 4, 2, mesh.shape["sec"]), OP + ("sec",))
    in_specs = (
        P("sec", OP, None),
        P(OP, "sec", None, None),
        P(OP, "sec", None, None),
        P(OP, "sec"),
        P("sec"),
    )
    out_specs = P("sec", OP, None)
    return jax.shard_map(sigma_rows, mesh=finer, in_specs=in_specs, out_specs=out_specs, check_vma=False)
```

```python
import jax
import jax.numpy as jnp
from jax import lax
from jax.experimental import pallas as pl
from jax.experimental.pallas import tpu as pltpu
from jax.sharding import Mesh
from jax.sharding import PartitionSpec as P

OP = ("x", "y", "c")
F32 = jnp.float32
BF16 = jnp.bfloat16


def exchanged(x, axis):
    return lax.all_to_all(x, axis, split_axis=0, concat_axis=0, tiled=True)


def shared(x, axis):
    return exchanged(jnp.broadcast_to(x[None], (lax.axis_size(axis),) + x.shape), axis)


def from_partner(x):
    return lax.ppermute(x, "c", [(0, 1), (1, 0)])


def around(x):
    n = lax.axis_size("sec")
    return lax.ppermute(x, "sec", [(n - 1, 0)])


def ahead(x):
    n = lax.axis_size("sec")
    return lax.ppermute(x, "sec", [(i, i + 1) for i in range(n - 1)])


def in_vmem(x):
    return pltpu.with_memory_space_constraint(x, pltpu.VMEM)


def in_hbm(x):
    return pltpu.with_memory_space_constraint(x, pltpu.HBM)


def fetch_kernel(where_ref, left_ref, right_ref, rows_ref, rights_ref, sems):
    kdev, sdev = right_ref.shape[:2]
    core = where_ref[1]
    fetches = []
    for k in range(kdev):
        for s in range(sdev):
            fetches.append(pltpu.make_async_copy(left_ref.at[k, s, :, core], rows_ref.at[s, k], sems.at[s, k]))
        fetches.append(pltpu.make_async_copy(right_ref.at[k, 0], rights_ref.at[k], sems.at[sdev, k]))
    for fetch in fetches:
        fetch.start()
    for fetch in fetches:
        fetch.wait()


def fetched(where, left, right):
    kdev, sdev, chips, _, tall, width = left.shape
    hbm = pl.BlockSpec(memory_space=pltpu.HBM)
    return pl.pallas_call(
        fetch_kernel,
        in_specs=[pl.BlockSpec(memory_space=pltpu.SMEM), hbm, hbm],
        out_specs=[pl.BlockSpec(memory_space=pltpu.VMEM)] * 2,
        out_shape=[
            pltpu.VMEM((sdev, kdev, chips, tall, width), BF16),
            pltpu.VMEM((kdev, width, width), BF16),
        ],
        scratch_shapes=[pltpu.SemaphoreType.DMA((sdev + 1, kdev))],
        compiler_params=pltpu.CompilerParams(vmem_limit_bytes=2**20),
        name="fetch",
    )(where, in_hbm(left), in_hbm(right))


def sums_kernel(where_ref, conn_ref, conn2_ref, dims_ref, near_ref, far_ref, rows0_ref, right0_ref, right_ref, left2_ref, right2_ref, own_ref, onward_ref, psi_ref, rows_ref, rights_ref, half_ref, sum_ref, staged_ref, sems, out_sem):
    kdev, sdev, width, _ = right_ref.shape
    chips, _, tall, _ = near_ref.shape
    group = where_ref[0]
    core = where_ref[1]
    many = chips * tall
    steps = [(0, 0, rows0_ref.at[0], right0_ref, ())]
    for whose, s in ((0, 1), (1, 0), (1, 1)):
        n = len(steps) - 1
        rights = (right_ref, right2_ref)[whose]
        fetches = []
        rows = rows0_ref.at[s]
        for k in range(kdev):
            if whose == 1:
                rows = rows_ref.at[s]
                fetches.append(pltpu.make_async_copy(left2_ref.at[k, s, :, core], rows.at[k], sems.at[0, n, k]))
            fetches.append(pltpu.make_async_copy(rights.at[k, s], rights_ref.at[n, k], sems.at[1, n, k]))
        for fetch in fetches:
            fetch.start()
        steps.append((whose, s, rows, rights_ref.at[n], fetches))
    cols = lax.broadcasted_iota(jnp.int32, (tall, width), 1)
    row = lax.broadcasted_iota(jnp.int32, (tall, width), 0)

    @pl.loop(0, chips)
    def _(chip):
        for s in range(sdev):
            size = dims_ref[s]
            for ref, seat in ((near_ref, core), (far_ref, 1 - core)):
                start = pl.multiple_of((chip * 2 + seat) * tall, tall)
                kept = (cols < size) & (row + start < size)
                psi_ref[s, pl.ds(start, tall), :] = jnp.where(kept, ref[chip, s].astype(F32), 0.0).astype(BF16)

    sum_ref[...] = jnp.zeros_like(sum_ref)
    for whose, s, rows, rights, fetches in steps:
        for fetch in fetches:
            fetch.wait()
        left = rows[...].reshape(kdev * many, width)
        half_ref[...] = jnp.dot(left, psi_ref[s], preferred_element_type=F32).astype(BF16)
        for k in range(kdev):
            target = (conn_ref, conn2_ref)[whose][k, s]
            place = target % sdev + jnp.where(target // sdev != group, sdev, 0)
            sum_ref[place] += lax.dot_general(
                half_ref[k * many : (k + 1) * many, :],
                rights[k],
                (((1,), (1,)), ((), ())),
                preferred_element_type=F32,
            )
    for chip in range(chips):
        for t in range(sdev):
            staged_ref[chip, t] = sum_ref[t, chip * tall : (chip + 1) * tall, :].astype(BF16)
    leave = pltpu.make_async_copy(staged_ref, own_ref, out_sem)
    leave.start()

    @pl.loop(0, chips)
    def _(chip):
        start = pl.multiple_of(chip * tall, tall)
        for t in range(sdev):
            onward_ref[chip, t] = sum_ref[sdev + t, pl.ds(start, tall), :].astype(BF16)

    leave.wait()


def slot_sums(where, conn, conn2, dims, near, far, rows0, right0, right, left2, right2):
    kdev, sdev, chips, _, tall, width = left2.shape
    assert sdev == 2
    rest = 2 * sdev - 1
    block = (chips, sdev, tall, width)
    smem = pl.BlockSpec(memory_space=pltpu.SMEM)
    vmem = pl.BlockSpec(memory_space=pltpu.VMEM)
    hbm = pl.BlockSpec(memory_space=pltpu.HBM)
    many = chips * tall
    return pl.pallas_call(
        sums_kernel,
        in_specs=[smem] * 4 + [vmem] * 4 + [hbm] * 3,
        out_specs=[hbm, vmem],
        out_shape=[pltpu.HBM(block, BF16), pltpu.VMEM(block, BF16)],
        scratch_shapes=[
            pltpu.VMEM((sdev, width, width), BF16),
            pltpu.VMEM((sdev, kdev, chips, tall, width), BF16),
            pltpu.VMEM((rest, kdev, width, width), BF16),
            pltpu.VMEM((kdev * many, width), BF16),
            pltpu.VMEM((2 * sdev, many, width), F32),
            pltpu.VMEM(block, BF16),
            pltpu.SemaphoreType.DMA((2, rest, kdev)),
            pltpu.SemaphoreType.DMA,
        ],
        compiler_params=pltpu.CompilerParams(vmem_limit_bytes=24 * 2**20),
        name="slot_sums",
    )(where, conn, conn2, dims, *(in_vmem(x) for x in (near, far, rows0, right0)), *(in_hbm(x) for x in (right, left2, right2)))


def kept_entries(dims, row_start, rows, width):
    row_ids = row_start + jnp.arange(rows, dtype=jnp.int32)
    col_ids = jnp.arange(width, dtype=jnp.int32)
    return (row_ids[None, :, None] < dims[:, None, None]) & (
        col_ids[None, None, :] < dims[:, None, None]
    )


def sigma_rows(psi, left_ops, right_ops, conn, dims):
    sdev, tall, width = psi.shape
    nx, ny = lax.axis_size("x"), lax.axis_size("y")
    places = (lax.axis_index("sec"), lax.axis_index("c"), lax.axis_index(OP) * tall)
    where = jnp.stack(places).astype(jnp.int32)
    by_row = left_ops.shape[:2] + (nx * ny, 2, tall, width)
    left2 = from_partner(left_ops).reshape(by_row)
    right2 = from_partner(right_ops)
    conn2 = from_partner(conn)
    left = left_ops.reshape(by_row)
    rows0, right0 = fetched(where, left, right_ops)
    by_y = shared(psi, "y").reshape(ny, sdev, tall, width)
    by_x = shared(by_y, "x").reshape(nx * ny, sdev, tall, width)
    kept = kept_entries(dims, places[2], tall, width)
    by_x, kept = lax.optimization_barrier((by_x, kept))
    other = from_partner(by_x)
    own, onward = slot_sums(where, conn, conn2, dims, by_x, other, rows0, right0, right_ops, left2, right2)
    by_chip = (nx, ny, sdev, tall, width)
    onward = exchanged(onward, "x").reshape(by_chip).astype(F32).sum(axis=0).astype(BF16)
    far = around(onward)
    near = ahead(onward)
    own = exchanged(own, "x").reshape(by_chip).astype(F32).sum(axis=0)
    summed = exchanged((own + far.astype(F32) + near.astype(F32)).astype(BF16), "y").astype(F32).sum(axis=0)
    return jnp.where(kept, summed, jnp.zeros_like(summed)).astype(BF16)


def solution(mesh):
    finer = Mesh(mesh.devices.reshape(4, 4, 2, mesh.shape["sec"]), OP + ("sec",))
    in_specs = (
        P("sec", OP, None),
        P(OP, "sec", None, None),
        P(OP, "sec", None, None),
        P(OP, "sec"),
        P("sec"),
    )
    out_specs = P("sec", OP, None)
    return jax.shard_map(sigma_rows, mesh=finer, in_specs=in_specs, out_specs=out_specs, check_vma=False)
```

```python
import jax
import jax.numpy as jnp
from jax import lax
from jax.experimental import pallas as pl
from jax.experimental.pallas import tpu as pltpu
from jax.sharding import Mesh
from jax.sharding import PartitionSpec as P

OP = ("x", "y", "c")
F32 = jnp.float32
BF16 = jnp.bfloat16


def exchanged(x, axis):
    return lax.all_to_all(x, axis, split_axis=0, concat_axis=0, tiled=True)


def shared(x, axis):
    return exchanged(jnp.broadcast_to(x[None], (lax.axis_size(axis),) + x.shape), axis)


def from_partner(x):
    return lax.ppermute(x, "c", [(0, 1), (1, 0)])


def around(x):
    n = lax.axis_size("sec")
    return lax.ppermute(x, "sec", [(n - 1, 0)])


def ahead(x):
    n = lax.axis_size("sec")
    return lax.ppermute(x, "sec", [(i, i + 1) for i in range(n - 1)])


def in_vmem(x):
    return pltpu.with_memory_space_constraint(x, pltpu.VMEM)


def in_hbm(x):
    return pltpu.with_memory_space_constraint(x, pltpu.HBM)


def fetch_kernel(where_ref, left_ref, right_ref, rows_ref, rights_ref, sems):
    kdev, sdev = right_ref.shape[:2]
    core = where_ref[1]
    fetches = []
    for k in range(kdev):
        for s in range(sdev):
            fetches.append(pltpu.make_async_copy(left_ref.at[k, s, :, core], rows_ref.at[s, k], sems.at[s, k]))
        fetches.append(pltpu.make_async_copy(right_ref.at[k, 0], rights_ref.at[k], sems.at[sdev, k]))
    for fetch in fetches:
        fetch.start()
    for fetch in fetches:
        fetch.wait()


def fetched(where, left, right):
    kdev, sdev, chips, _, tall, width = left.shape
    hbm = pl.BlockSpec(memory_space=pltpu.HBM)
    return pl.pallas_call(
        fetch_kernel,
        in_specs=[pl.BlockSpec(memory_space=pltpu.SMEM), hbm, hbm],
        out_specs=[pl.BlockSpec(memory_space=pltpu.VMEM)] * 2,
        out_shape=[
            pltpu.VMEM((sdev, kdev, chips, tall, width), BF16),
            pltpu.VMEM((kdev, width, width), BF16),
        ],
        scratch_shapes=[pltpu.SemaphoreType.DMA((sdev + 1, kdev))],
        compiler_params=pltpu.CompilerParams(vmem_limit_bytes=2**20),
        name="fetch",
    )(where, in_hbm(left), in_hbm(right))


def sums_kernel(where_ref, conn_ref, conn2_ref, dims_ref, near_ref, far_ref, rows0_ref, right0_ref, right_ref, left2_ref, right2_ref, own_ref, onward_ref, psi_ref, rows_ref, rights_ref, half_ref, sum_ref, staged_ref, sems, out_sem):
    kdev, sdev, width, _ = right_ref.shape
    chips, _, tall, _ = near_ref.shape
    group = where_ref[0]
    core = where_ref[1]
    many = chips * tall
    steps = [(0, 0, rows0_ref.at[0], right0_ref, ())]
    for whose, s in ((0, 1), (1, 0), (1, 1)):
        n = len(steps) - 1
        rights = (right_ref, right2_ref)[whose]
        fetches = []
        rows = rows0_ref.at[s]
        for k in range(kdev):
            if whose == 1:
                rows = rows_ref.at[s]
                fetches.append(pltpu.make_async_copy(left2_ref.at[k, s, :, core], rows.at[k], sems.at[0, n, k]))
            fetches.append(pltpu.make_async_copy(rights.at[k, s], rights_ref.at[n, k], sems.at[1, n, k]))
        for fetch in fetches:
            fetch.start()
        steps.append((whose, s, rows, rights_ref.at[n], fetches))
    cols = lax.broadcasted_iota(jnp.int32, (tall, width), 1)
    row = lax.broadcasted_iota(jnp.int32, (tall, width), 0)

    def mask_chip(s, chip):
        size = dims_ref[s]
        for ref, seat in ((near_ref, core), (far_ref, 1 - core)):
            start = pl.multiple_of((chip * 2 + seat) * tall, tall)
            kept = (cols < size) & (row + start < size)
            psi_ref[s, pl.ds(start, tall), :] = jnp.where(kept, ref[chip, s].astype(F32), 0.0).astype(BF16)

    @pl.loop(0, chips // 2)
    def _(pair):
        mask_chip(0, 2 * pair)
        mask_chip(0, 2 * pair + 1)

    for s in range(1, sdev):
        for chip in range(chips):
            mask_chip(s, chip)
    sum_ref[...] = jnp.zeros_like(sum_ref)
    for whose, s, rows, rights, fetches in steps:
        for fetch in fetches:
            fetch.wait()
        left = rows[...].reshape(kdev * many, width)
        half_ref[...] = jnp.dot(left, psi_ref[s], preferred_element_type=F32).astype(BF16)
        for k in range(kdev):
            target = (conn_ref, conn2_ref)[whose][k, s]
            place = target % sdev + jnp.where(target // sdev != group, sdev, 0)
            sum_ref[place] += lax.dot_general(
                half_ref[k * many : (k + 1) * many, :],
                rights[k],
                (((1,), (1,)), ((), ())),
                preferred_element_type=F32,
            )
    for chip in range(chips):
        for t in range(sdev):
            staged_ref[chip, t] = sum_ref[t, chip * tall : (chip + 1) * tall, :].astype(BF16)
    leave = pltpu.make_async_copy(staged_ref, own_ref, out_sem)
    leave.start()

    @pl.loop(0, chips)
    def _(chip):
        start = pl.multiple_of(chip * tall, tall)
        for t in range(sdev):
            onward_ref[chip, t] = sum_ref[sdev + t, pl.ds(start, tall), :].astype(BF16)

    leave.wait()


def slot_sums(where, conn, conn2, dims, near, far, rows0, right0, right, left2, right2):
    kdev, sdev, chips, _, tall, width = left2.shape
    assert sdev == 2
    rest = 2 * sdev - 1
    block = (chips, sdev, tall, width)
    smem = pl.BlockSpec(memory_space=pltpu.SMEM)
    vmem = pl.BlockSpec(memory_space=pltpu.VMEM)
    hbm = pl.BlockSpec(memory_space=pltpu.HBM)
    many = chips * tall
    return pl.pallas_call(
        sums_kernel,
        in_specs=[smem] * 4 + [vmem] * 4 + [hbm] * 3,
        out_specs=[hbm, vmem],
        out_shape=[pltpu.HBM(block, BF16), pltpu.VMEM(block, BF16)],
        scratch_shapes=[
            pltpu.VMEM((sdev, width, width), BF16),
            pltpu.VMEM((sdev, kdev, chips, tall, width), BF16),
            pltpu.VMEM((rest, kdev, width, width), BF16),
            pltpu.VMEM((kdev * many, width), BF16),
            pltpu.VMEM((2 * sdev, many, width), F32),
            pltpu.VMEM(block, BF16),
            pltpu.SemaphoreType.DMA((2, rest, kdev)),
            pltpu.SemaphoreType.DMA,
        ],
        compiler_params=pltpu.CompilerParams(vmem_limit_bytes=24 * 2**20),
        name="slot_sums",
    )(where, conn, conn2, dims, *(in_vmem(x) for x in (near, far, rows0, right0)), *(in_hbm(x) for x in (right, left2, right2)))


def kept_entries(dims, row_start, rows, width):
    row_ids = row_start + jnp.arange(rows, dtype=jnp.int32)
    col_ids = jnp.arange(width, dtype=jnp.int32)
    return (row_ids[None, :, None] < dims[:, None, None]) & (
        col_ids[None, None, :] < dims[:, None, None]
    )


def sigma_rows(psi, left_ops, right_ops, conn, dims):
    sdev, tall, width = psi.shape
    nx, ny = lax.axis_size("x"), lax.axis_size("y")
    places = (lax.axis_index("sec"), lax.axis_index("c"), lax.axis_index(OP) * tall)
    where = jnp.stack(places).astype(jnp.int32)
    by_row = left_ops.shape[:2] + (nx * ny, 2, tall, width)
    left2 = from_partner(left_ops).reshape(by_row)
    right2 = from_partner(right_ops)
    conn2 = from_partner(conn)
    left = left_ops.reshape(by_row)
    rows0, right0 = fetched(where, left, right_ops)
    by_y = shared(psi, "y").reshape(ny, sdev, tall, width)
    by_x = shared(by_y, "x").reshape(nx * ny, sdev, tall, width)
    kept = kept_entries(dims, places[2], tall, width)
    by_x, kept = lax.optimization_barrier((by_x, kept))
    other = from_partner(by_x)
    own, onward = slot_sums(where, conn, conn2, dims, by_x, other, rows0, right0, right_ops, left2, right2)
    by_chip = (nx, ny, sdev, tall, width)
    onward = exchanged(onward, "x").reshape(by_chip).astype(F32).sum(axis=0).astype(BF16)
    far = around(onward)
    near = ahead(onward)
    own = exchanged(own, "x").reshape(by_chip).astype(F32).sum(axis=0)
    summed = exchanged((own + far.astype(F32) + near.astype(F32)).astype(BF16), "y").astype(F32).sum(axis=0)
    return jnp.where(kept, summed, jnp.zeros_like(summed)).astype(BF16)


def solution(mesh):
    finer = Mesh(mesh.devices.reshape(4, 4, 2, mesh.shape["sec"]), OP + ("sec",))
    in_specs = (
        P("sec", OP, None),
        P(OP, "sec", None, None),
        P(OP, "sec", None, None),
        P(OP, "sec"),
        P("sec"),
    )
    out_specs = P("sec", OP, None)
    return jax.shard_map(sigma_rows, mesh=finer, in_specs=in_specs, out_specs=out_specs, check_vma=False)
```

```python
import jax
import jax.numpy as jnp
from jax import lax
from jax.experimental import pallas as pl
from jax.experimental.pallas import tpu as pltpu
from jax.sharding import Mesh
from jax.sharding import PartitionSpec as P

OP = ("x", "y", "c")
F32 = jnp.float32
BF16 = jnp.bfloat16


def exchanged(x, axis):
    return lax.all_to_all(x, axis, split_axis=0, concat_axis=0, tiled=True)


def shared(x, axis):
    return exchanged(jnp.broadcast_to(x[None], (lax.axis_size(axis),) + x.shape), axis)


def from_partner(x):
    return lax.ppermute(x, "c", [(0, 1), (1, 0)])


def around(x):
    n = lax.axis_size("sec")
    return lax.ppermute(x, "sec", [(n - 1, 0)])


def ahead(x):
    n = lax.axis_size("sec")
    return lax.ppermute(x, "sec", [(i, i + 1) for i in range(n - 1)])


def in_vmem(x):
    return pltpu.with_memory_space_constraint(x, pltpu.VMEM)


def in_hbm(x):
    return pltpu.with_memory_space_constraint(x, pltpu.HBM)


def sums_kernel(where_ref, conn_ref, conn2_ref, dims_ref, near_ref, far_ref, right_ref, left_ref, left2_ref, right2_ref, own_ref, onward_ref, psi_ref, rows_ref, rights_ref, half_ref, sum_ref, staged_ref, sems, out_sem):
    kdev, sdev, width, _ = right_ref.shape
    chips, _, tall, _ = near_ref.shape
    group = where_ref[0]
    core = where_ref[1]
    many = chips * tall
    steps = []
    for n, (whose, s) in enumerate(((0, 0), (0, 1), (1, 0), (1, 1))):
        fetches = []
        for k in range(kdev):
            source = (left_ref, left2_ref)[whose].at[k, s, :, core]
            fetches.append(pltpu.make_async_copy(source, rows_ref.at[n, k], sems.at[n, k]))
        rights = right_ref.at[:, s]
        if whose == 1:
            rights = rights_ref.at[:, s]
            for k in range(kdev):
                fetches.append(pltpu.make_async_copy(right2_ref.at[k, s], rights_ref.at[k, s], sems.at[2 * sdev + s, k]))
        for fetch in fetches:
            fetch.start()
        steps.append((whose, s, rows_ref.at[n], rights, fetches))
    cols = lax.broadcasted_iota(jnp.int32, (tall, width), 1)
    row = lax.broadcasted_iota(jnp.int32, (tall, width), 0)

    def mask_chip(s, chip):
        size = dims_ref[s]
        for ref, seat in ((near_ref, core), (far_ref, 1 - core)):
            start = pl.multiple_of((chip * 2 + seat) * tall, tall)
            kept = (cols < size) & (row + start < size)
            psi_ref[s, pl.ds(start, tall), :] = jnp.where(kept, ref[chip, s].astype(F32), 0.0).astype(BF16)

    @pl.loop(0, chips // 2)
    def _(pair):
        mask_chip(0, 2 * pair)
        mask_chip(0, 2 * pair + 1)

    for s in range(1, sdev):
        for chip in range(chips):
            mask_chip(s, chip)
    sum_ref[...] = jnp.zeros_like(sum_ref)
    for whose, s, rows, rights, fetches in steps:
        for fetch in fetches:
            fetch.wait()
        left = rows[...].reshape(kdev * many, width)
        half_ref[...] = jnp.dot(left, psi_ref[s], preferred_element_type=F32).astype(BF16)
        for k in range(kdev):
            target = (conn_ref, conn2_ref)[whose][k, s]
            place = target % sdev + jnp.where(target // sdev != group, sdev, 0)
            sum_ref[place] += lax.dot_general(
                half_ref[k * many : (k + 1) * many, :],
                rights[k],
                (((1,), (1,)), ((), ())),
                preferred_element_type=F32,
            )
    for chip in range(chips):
        for t in range(sdev):
            staged_ref[chip, t] = sum_ref[t, chip * tall : (chip + 1) * tall, :].astype(BF16)
    leave = pltpu.make_async_copy(staged_ref, own_ref, out_sem)
    leave.start()

    @pl.loop(0, chips)
    def _(chip):
        start = pl.multiple_of(chip * tall, tall)
        for t in range(sdev):
            onward_ref[chip, t] = sum_ref[sdev + t, pl.ds(start, tall), :].astype(BF16)

    leave.wait()


def slot_sums(where, conn, conn2, dims, near, far, right, left, left2, right2):
    kdev, sdev, chips, _, tall, width = left2.shape
    assert sdev == 2
    block = (chips, sdev, tall, width)
    smem = pl.BlockSpec(memory_space=pltpu.SMEM)
    vmem = pl.BlockSpec(memory_space=pltpu.VMEM)
    hbm = pl.BlockSpec(memory_space=pltpu.HBM)
    many = chips * tall
    return pl.pallas_call(
        sums_kernel,
        in_specs=[smem] * 4 + [vmem] * 3 + [hbm] * 3,
        out_specs=[hbm, vmem],
        out_shape=[pltpu.HBM(block, BF16), pltpu.VMEM(block, BF16)],
        scratch_shapes=[
            pltpu.VMEM((sdev, width, width), BF16),
            pltpu.VMEM((2 * sdev, kdev, chips, tall, width), BF16),
            pltpu.VMEM((kdev, sdev, width, width), BF16),
            pltpu.VMEM((kdev * many, width), BF16),
            pltpu.VMEM((2 * sdev, many, width), F32),
            pltpu.VMEM(block, BF16),
            pltpu.SemaphoreType.DMA((3 * sdev, kdev)),
            pltpu.SemaphoreType.DMA,
        ],
        compiler_params=pltpu.CompilerParams(vmem_limit_bytes=24 * 2**20),
        name="slot_sums",
    )(where, conn, conn2, dims, *(in_vmem(x) for x in (near, far, right)), *(in_hbm(x) for x in (left, left2, right2)))


def kept_entries(dims, row_start, rows, width):
    row_ids = row_start + jnp.arange(rows, dtype=jnp.int32)
    col_ids = jnp.arange(width, dtype=jnp.int32)
    return (row_ids[None, :, None] < dims[:, None, None]) & (
        col_ids[None, None, :] < dims[:, None, None]
    )


def sigma_rows(psi, left_ops, right_ops, conn, dims):
    sdev, tall, width = psi.shape
    nx, ny = lax.axis_size("x"), lax.axis_size("y")
    places = (lax.axis_index("sec"), lax.axis_index("c"), lax.axis_index(OP) * tall)
    where = jnp.stack(places).astype(jnp.int32)
    by_row = left_ops.shape[:2] + (nx * ny, 2, tall, width)
    left2 = from_partner(left_ops).reshape(by_row)
    right2 = from_partner(right_ops)
    conn2 = from_partner(conn)
    by_y = shared(psi, "y").reshape(ny, sdev, tall, width)
    by_x = shared(by_y, "x").reshape(nx * ny, sdev, tall, width)
    kept = kept_entries(dims, places[2], tall, width)
    by_x, kept = lax.optimization_barrier((by_x, kept))
    other = from_partner(by_x)
    own, onward = slot_sums(where, conn, conn2, dims, by_x, other, right_ops, left_ops.reshape(by_row), left2, right2)
    by_chip = (nx, ny, sdev, tall, width)
    onward = exchanged(onward, "x").reshape(by_chip).astype(F32).sum(axis=0).astype(BF16)
    far = around(onward)
    near = ahead(onward)
    own = exchanged(own, "x").reshape(by_chip).astype(F32).sum(axis=0)
    summed = exchanged((own + far.astype(F32) + near.astype(F32)).astype(BF16), "y").astype(F32).sum(axis=0)
    return jnp.where(kept, summed, jnp.zeros_like(summed)).astype(BF16)


def solution(mesh):
    finer = Mesh(mesh.devices.reshape(4, 4, 2, mesh.shape["sec"]), OP + ("sec",))
    in_specs = (
        P("sec", OP, None),
        P(OP, "sec", None, None),
        P(OP, "sec", None, None),
        P(OP, "sec"),
        P("sec"),
    )
    out_specs = P("sec", OP, None)
    return jax.shard_map(sigma_rows, mesh=finer, in_specs=in_specs, out_specs=out_specs, check_vma=False)
```

```python
import jax
import jax.numpy as jnp
from jax import lax
from jax.experimental import pallas as pl
from jax.experimental.pallas import tpu as pltpu
from jax.sharding import Mesh
from jax.sharding import PartitionSpec as P

OP = ("x", "y", "c")
F32 = jnp.float32
BF16 = jnp.bfloat16


def exchanged(x, axis):
    return lax.all_to_all(x, axis, split_axis=0, concat_axis=0, tiled=True)


def shared(x, axis):
    return exchanged(jnp.broadcast_to(x[None], (lax.axis_size(axis),) + x.shape), axis)


def from_partner(x):
    return lax.ppermute(x, "c", [(0, 1), (1, 0)])


def around(x):
    n = lax.axis_size("sec")
    return lax.ppermute(x, "sec", [(n - 1, 0)])


def ahead(x):
    n = lax.axis_size("sec")
    return lax.ppermute(x, "sec", [(i, i + 1) for i in range(n - 1)])


def in_vmem(x):
    return pltpu.with_memory_space_constraint(x, pltpu.VMEM)


def in_hbm(x):
    return pltpu.with_memory_space_constraint(x, pltpu.HBM)


def sums_kernel(where_ref, conn_ref, conn2_ref, dims_ref, near_ref, far_ref, left_ref, right_ref, left2_ref, right2_ref, own_ref, onward_ref, psi_ref, rows_ref, rights_ref, half_ref, sum_ref, staged_ref, sems, out_sem):
    kdev, sdev, width, _ = right_ref.shape
    chips, _, tall, _ = near_ref.shape
    group = where_ref[0]
    core = where_ref[1]
    many = chips * tall
    fetches = {}
    for whose in range(2):
        for s in range(sdev):
            copies = []
            for k in range(kdev):
                n = (whose * sdev + s) * kdev + k
                if whose == 1:
                    rows = rows_ref.at[whose, s, k]
                    copies.append(pltpu.make_async_copy(left2_ref.at[k, s, :, core], rows, sems.at[0, n]))
                right = (right_ref, right2_ref)[whose].at[k, s]
                copies.append(pltpu.make_async_copy(right, rights_ref.at[whose, s, k], sems.at[1, n]))
            for fetch in copies:
                fetch.start()
            fetches[whose, s] = copies
    cols = lax.broadcasted_iota(jnp.int32, (tall, width), 1)
    row = lax.broadcasted_iota(jnp.int32, (tall, width), 0)

    @pl.loop(0, chips)
    def _(chip):
        for s in range(sdev):
            size = dims_ref[s]
            for ref, seat in ((near_ref, core), (far_ref, 1 - core)):
                start = pl.multiple_of((chip * 2 + seat) * tall, tall)
                kept = (cols < size) & (row + start < size)
                psi_ref[s, pl.ds(start, tall), :] = jnp.where(kept, ref[chip, s].astype(F32), 0.0).astype(BF16)
            for k in range(kdev):
                rows_ref[0, s, k, chip] = left_ref[k, s, chip, core]

    sum_ref[...] = jnp.zeros_like(sum_ref)

    def first_product(whose, s):
        left = rows_ref[whose, s].reshape(kdev * many, width)
        half_ref[s] = jnp.dot(left, psi_ref[s], preferred_element_type=F32).astype(BF16)

    def second_product(whose, s):
        for k in range(kdev):
            target = (conn_ref, conn2_ref)[whose][k, s]
            place = target % sdev + jnp.where(target // sdev != group, sdev, 0)
            sum_ref[place] += lax.dot_general(
                half_ref[s, k * many : (k + 1) * many, :],
                rights_ref[whose, s, k],
                (((1,), (1,)), ((), ())),
                preferred_element_type=F32,
            )

    for s in range(sdev):
        first_product(0, s)
    for s in range(sdev):
        for fetch in fetches[0, s]:
            fetch.wait()
        second_product(0, s)
    for s in range(sdev):
        for fetch in fetches[1, s]:
            fetch.wait()
        first_product(1, s)
        second_product(1, s)
    for chip in range(chips):
        for t in range(sdev):
            staged_ref[chip, t] = sum_ref[t, chip * tall : (chip + 1) * tall, :].astype(BF16)
    leave = pltpu.make_async_copy(staged_ref, own_ref, out_sem)
    leave.start()

    @pl.loop(0, chips)
    def _(chip):
        start = pl.multiple_of(chip * tall, tall)
        for t in range(sdev):
            onward_ref[chip, t] = sum_ref[sdev + t, pl.ds(start, tall), :].astype(BF16)

    leave.wait()


def slot_sums(where, conn, conn2, dims, near, far, left, right, left2, right2):
    kdev, sdev, chips, _, tall, width = left2.shape
    assert sdev == 2
    block = (chips, sdev, tall, width)
    smem = pl.BlockSpec(memory_space=pltpu.SMEM)
    vmem = pl.BlockSpec(memory_space=pltpu.VMEM)
    hbm = pl.BlockSpec(memory_space=pltpu.HBM)
    many = chips * tall
    return pl.pallas_call(
        sums_kernel,
        in_specs=[smem] * 4 + [vmem] * 3 + [hbm] * 3,
        out_specs=[hbm, vmem],
        out_shape=[pltpu.HBM(block, BF16), pltpu.VMEM(block, BF16)],
        scratch_shapes=[
            pltpu.VMEM((sdev, width, width), BF16),
            pltpu.VMEM((2, sdev, kdev, chips, tall, width), BF16),
            pltpu.VMEM((2, sdev, kdev, width, width), BF16),
            pltpu.VMEM((sdev, kdev * many, width), BF16),
            pltpu.VMEM((2 * sdev, many, width), F32),
            pltpu.VMEM(block, BF16),
            pltpu.SemaphoreType.DMA((2, 2 * sdev * kdev)),
            pltpu.SemaphoreType.DMA,
        ],
        compiler_params=pltpu.CompilerParams(vmem_limit_bytes=24 * 2**20),
        name="slot_sums",
    )(where, conn, conn2, dims, *(in_vmem(x) for x in (near, far, left)), *(in_hbm(x) for x in (right, left2, right2)))


def kept_entries(dims, row_start, rows, width):
    row_ids = row_start + jnp.arange(rows, dtype=jnp.int32)
    col_ids = jnp.arange(width, dtype=jnp.int32)
    return (row_ids[None, :, None] < dims[:, None, None]) & (
        col_ids[None, None, :] < dims[:, None, None]
    )


def sigma_rows(psi, left_ops, right_ops, conn, dims):
    sdev, tall, width = psi.shape
    nx, ny = lax.axis_size("x"), lax.axis_size("y")
    places = (lax.axis_index("sec"), lax.axis_index("c"), lax.axis_index(OP) * tall)
    where = jnp.stack(places).astype(jnp.int32)
    by_row = left_ops.shape[:2] + (nx * ny, 2, tall, width)
    left2 = from_partner(left_ops).reshape(by_row)
    right2 = from_partner(right_ops)
    conn2 = from_partner(conn)
    by_y = shared(psi, "y").reshape(ny, sdev, tall, width)
    by_x = shared(by_y, "x").reshape(nx * ny, sdev, tall, width)
    kept = kept_entries(dims, places[2], tall, width)
    by_x, kept = lax.optimization_barrier((by_x, kept))
    other = from_partner(by_x)
    own, onward = slot_sums(where, conn, conn2, dims, by_x, other, left_ops.reshape(by_row), right_ops, left2, right2)
    by_chip = (nx, ny, sdev, tall, width)
    onward = exchanged(onward, "x").reshape(by_chip).astype(F32).sum(axis=0).astype(BF16)
    far = around(onward)
    near = ahead(onward)
    own = exchanged(own, "x").reshape(by_chip).astype(F32).sum(axis=0)
    summed = exchanged((own + far.astype(F32) + near.astype(F32)).astype(BF16), "y").astype(F32).sum(axis=0)
    return jnp.where(kept, summed, jnp.zeros_like(summed)).astype(BF16)


def solution(mesh):
    finer = Mesh(mesh.devices.reshape(4, 4, 2, mesh.shape["sec"]), OP + ("sec",))
    in_specs = (
        P("sec", OP, None),
        P(OP, "sec", None, None),
        P(OP, "sec", None, None),
        P(OP, "sec"),
        P("sec"),
    )
    out_specs = P("sec", OP, None)
    return jax.shard_map(sigma_rows, mesh=finer, in_specs=in_specs, out_specs=out_specs, check_vma=False)
```

```python
import jax
import jax.numpy as jnp
from jax import lax
from jax.experimental import pallas as pl
from jax.experimental.pallas import tpu as pltpu
from jax.sharding import Mesh
from jax.sharding import PartitionSpec as P

OP = ("x", "y", "c")
F32 = jnp.float32
BF16 = jnp.bfloat16


def exchanged(x, axis):
    return lax.all_to_all(x, axis, split_axis=0, concat_axis=0, tiled=True)


def shared(x, axes, count):
    return exchanged(jnp.broadcast_to(x[None], (count,) + x.shape), axes)


def from_partner(x):
    return lax.ppermute(x, "c", [(0, 1), (1, 0)])


def around(x):
    n = lax.axis_size("sec")
    return lax.ppermute(x, "sec", [(n - 1, 0)])


def ahead(x):
    n = lax.axis_size("sec")
    return lax.ppermute(x, "sec", [(i, i + 1) for i in range(n - 1)])


def in_vmem(x):
    return pltpu.with_memory_space_constraint(x, pltpu.VMEM)


def in_hbm(x):
    return pltpu.with_memory_space_constraint(x, pltpu.HBM)


def fetch_kernel(where_ref, left_ref, right_ref, rows_ref, rights_ref, sems):
    kdev, sdev = right_ref.shape[:2]
    core = where_ref[1]
    fetches = []
    for k in range(kdev):
        for s in range(sdev):
            fetches.append(pltpu.make_async_copy(left_ref.at[k, s, :, core], rows_ref.at[s, k], sems.at[s, k]))
        fetches.append(pltpu.make_async_copy(right_ref.at[k, 0], rights_ref.at[k], sems.at[sdev, k]))
    for fetch in fetches:
        fetch.start()
    for fetch in fetches:
        fetch.wait()


def fetched(where, left, right):
    kdev, sdev, chips, _, tall, width = left.shape
    hbm = pl.BlockSpec(memory_space=pltpu.HBM)
    return pl.pallas_call(
        fetch_kernel,
        in_specs=[pl.BlockSpec(memory_space=pltpu.SMEM), hbm, hbm],
        out_specs=[pl.BlockSpec(memory_space=pltpu.VMEM)] * 2,
        out_shape=[
            pltpu.VMEM((sdev, kdev, chips, tall, width), BF16),
            pltpu.VMEM((kdev, width, width), BF16),
        ],
        scratch_shapes=[pltpu.SemaphoreType.DMA((sdev + 1, kdev))],
        compiler_params=pltpu.CompilerParams(vmem_limit_bytes=2**20),
        name="fetch",
    )(where, in_hbm(left), in_hbm(right))


def sums_kernel(where_ref, conn_ref, conn2_ref, dims_ref, near_ref, far_ref, rows0_ref, right0_ref, right_ref, left2_ref, right2_ref, own_ref, onward_ref, psi_ref, rows_ref, rights_ref, half_ref, sum_ref, staged_ref, sems, out_sem):
    kdev, sdev, width, _ = right_ref.shape
    chips, _, tall, _ = near_ref.shape
    group = where_ref[0]
    core = where_ref[1]
    many = chips * tall
    steps = [(0, 0, rows0_ref.at[0], right0_ref, ())]
    for whose, s in ((0, 1), (1, 0), (1, 1)):
        n = len(steps) - 1
        rights = (right_ref, right2_ref)[whose]
        fetches = []
        rows = rows0_ref.at[s]
        for k in range(kdev):
            if whose == 1:
                rows = rows_ref.at[s]
                fetches.append(pltpu.make_async_copy(left2_ref.at[k, s, :, core], rows.at[k], sems.at[0, n, k]))
            fetches.append(pltpu.make_async_copy(rights.at[k, s], rights_ref.at[n, k], sems.at[1, n, k]))
        for fetch in fetches:
            fetch.start()
        steps.append((whose, s, rows, rights_ref.at[n], fetches))
    cols = lax.broadcasted_iota(jnp.int32, (tall, width), 1)
    row = lax.broadcasted_iota(jnp.int32, (tall, width), 0)

    def mask_chip(s, chip):
        size = dims_ref[s]
        for ref, seat in ((near_ref, core), (far_ref, 1 - core)):
            start = pl.multiple_of((chip * 2 + seat) * tall, tall)
            kept = (cols < size) & (row + start < size)
            psi_ref[s, pl.ds(start, tall), :] = jnp.where(kept, ref[chip, s].astype(F32), 0.0).astype(BF16)

    @pl.loop(0, chips // 2)
    def _(pair):
        mask_chip(0, 2 * pair)
        mask_chip(0, 2 * pair + 1)

    for s in range(1, sdev):
        for chip in range(chips):
            mask_chip(s, chip)
    sum_ref[...] = jnp.zeros_like(sum_ref)
    for whose, s, rows, rights, fetches in steps:
        for fetch in fetches:
            fetch.wait()
        left = rows[...].reshape(kdev * many, width)
        half_ref[...] = jnp.dot(left, psi_ref[s], preferred_element_type=F32).astype(BF16)
        for k in range(kdev):
            target = (conn_ref, conn2_ref)[whose][k, s]
            place = target % sdev + jnp.where(target // sdev != group, sdev, 0)
            sum_ref[place] += lax.dot_general(
                half_ref[k * many : (k + 1) * many, :],
                rights[k],
                (((1,), (1,)), ((), ())),
                preferred_element_type=F32,
            )
    for chip in range(chips):
        for t in range(sdev):
            staged_ref[chip, t] = sum_ref[t, chip * tall : (chip + 1) * tall, :].astype(BF16)
    leave = pltpu.make_async_copy(staged_ref, own_ref, out_sem)
    leave.start()

    @pl.loop(0, chips)
    def _(chip):
        start = pl.multiple_of(chip * tall, tall)
        for t in range(sdev):
            onward_ref[chip, t] = sum_ref[sdev + t, pl.ds(start, tall), :].astype(BF16)

    leave.wait()


def slot_sums(where, conn, conn2, dims, near, far, rows0, right0, right, left2, right2):
    kdev, sdev, chips, _, tall, width = left2.shape
    assert sdev == 2
    rest = 2 * sdev - 1
    block = (chips, sdev, tall, width)
    smem = pl.BlockSpec(memory_space=pltpu.SMEM)
    vmem = pl.BlockSpec(memory_space=pltpu.VMEM)
    hbm = pl.BlockSpec(memory_space=pltpu.HBM)
    many = chips * tall
    return pl.pallas_call(
        sums_kernel,
        in_specs=[smem] * 4 + [vmem] * 4 + [hbm] * 3,
        out_specs=[hbm, vmem],
        out_shape=[pltpu.HBM(block, BF16), pltpu.VMEM(block, BF16)],
        scratch_shapes=[
            pltpu.VMEM((sdev, width, width), BF16),
            pltpu.VMEM((sdev, kdev, chips, tall, width), BF16),
            pltpu.VMEM((rest, kdev, width, width), BF16),
            pltpu.VMEM((kdev * many, width), BF16),
            pltpu.VMEM((2 * sdev, many, width), F32),
            pltpu.VMEM(block, BF16),
            pltpu.SemaphoreType.DMA((2, rest, kdev)),
            pltpu.SemaphoreType.DMA,
        ],
        compiler_params=pltpu.CompilerParams(vmem_limit_bytes=24 * 2**20),
        name="slot_sums",
    )(where, conn, conn2, dims, *(in_vmem(x) for x in (near, far, rows0, right0)), *(in_hbm(x) for x in (right, left2, right2)))


def kept_entries(dims, row_start, rows, width):
    row_ids = row_start + jnp.arange(rows, dtype=jnp.int32)
    col_ids = jnp.arange(width, dtype=jnp.int32)
    return (row_ids[None, :, None] < dims[:, None, None]) & (
        col_ids[None, None, :] < dims[:, None, None]
    )


def sigma_rows(psi, left_ops, right_ops, conn, dims):
    sdev, tall, width = psi.shape
    nx, ny = lax.axis_size("x"), lax.axis_size("y")
    places = (lax.axis_index("sec"), lax.axis_index("c"), lax.axis_index(OP) * tall)
    where = jnp.stack(places).astype(jnp.int32)
    by_row = left_ops.shape[:2] + (nx * ny, 2, tall, width)
    left2 = from_partner(left_ops).reshape(by_row)
    right2 = from_partner(right_ops)
    conn2 = from_partner(conn)
    left = left_ops.reshape(by_row)
    rows0, right0 = fetched(where, left, right_ops)
    by_x = shared(psi, ("x", "y"), nx * ny)
    kept = kept_entries(dims, places[2], tall, width)
    by_x, kept = lax.optimization_barrier((by_x, kept))
    other = from_partner(by_x)
    own, onward = slot_sums(where, conn, conn2, dims, by_x, other, rows0, right0, right_ops, left2, right2)
    by_chip = (nx, ny, sdev, tall, width)
    onward = exchanged(onward, "x").reshape(by_chip).astype(F32).sum(axis=0).astype(BF16)
    far = around(onward)
    near = ahead(onward)
    own = exchanged(own, "x").reshape(by_chip).astype(F32).sum(axis=0)
    summed = exchanged((own + far.astype(F32) + near.astype(F32)).astype(BF16), "y").astype(F32).sum(axis=0)
    return jnp.where(kept, summed, jnp.zeros_like(summed)).astype(BF16)


def solution(mesh):
    finer = Mesh(mesh.devices.reshape(4, 4, 2, mesh.shape["sec"]), OP + ("sec",))
    in_specs = (
        P("sec", OP, None),
        P(OP, "sec", None, None),
        P(OP, "sec", None, None),
        P(OP, "sec"),
        P("sec"),
    )
    out_specs = P("sec", OP, None)
    return jax.shard_map(sigma_rows, mesh=finer, in_specs=in_specs, out_specs=out_specs, check_vma=False)
```

```python
import functools

import jax
import jax.numpy as jnp
from jax import lax
from jax.experimental import pallas as pl
from jax.experimental.pallas import tpu as pltpu
from jax.sharding import Mesh
from jax.sharding import PartitionSpec as P

OP = ("x", "y", "c")
F32 = jnp.float32
BF16 = jnp.bfloat16


def exchanged(x, axis):
    return lax.all_to_all(x, axis, split_axis=0, concat_axis=0, tiled=True)


def shared(x, axes, count):
    return exchanged(jnp.broadcast_to(x[None], (count,) + x.shape), axes)


def from_partner(x):
    return lax.ppermute(x, "c", [(0, 1), (1, 0)])


def around(x):
    n = lax.axis_size("sec")
    return lax.ppermute(x, "sec", [(n - 1, 0)])


def ahead(x):
    n = lax.axis_size("sec")
    return lax.ppermute(x, "sec", [(i, i + 1) for i in range(n - 1)])


def in_vmem(x):
    return pltpu.with_memory_space_constraint(x, pltpu.VMEM)


def in_hbm(x):
    return pltpu.with_memory_space_constraint(x, pltpu.HBM)


def fetch_kernel(where_ref, left_ref, right_ref, rows_ref, rights_ref, sems):
    kdev, sdev = right_ref.shape[:2]
    core = where_ref[1]
    fetches = []
    for k in range(kdev):
        for s in range(sdev):
            fetches.append(pltpu.make_async_copy(left_ref.at[k, s, :, core], rows_ref.at[s, k], sems.at[s, k]))
        fetches.append(pltpu.make_async_copy(right_ref.at[k, 0], rights_ref.at[k], sems.at[sdev, k]))
    for fetch in fetches:
        fetch.start()
    for fetch in fetches:
        fetch.wait()


def fetched(where, left, right):
    kdev, sdev, chips, _, tall, width = left.shape
    hbm = pl.BlockSpec(memory_space=pltpu.HBM)
    return pl.pallas_call(
        fetch_kernel,
        in_specs=[pl.BlockSpec(memory_space=pltpu.SMEM), hbm, hbm],
        out_specs=[pl.BlockSpec(memory_space=pltpu.VMEM)] * 2,
        out_shape=[
            pltpu.VMEM((sdev, kdev, chips, tall, width), BF16),
            pltpu.VMEM((kdev, width, width), BF16),
        ],
        scratch_shapes=[pltpu.SemaphoreType.DMA((sdev + 1, kdev))],
        compiler_params=pltpu.CompilerParams(vmem_limit_bytes=2**20),
        name="fetch",
    )(where, in_hbm(left), in_hbm(right))


def sums_kernel(nx, ny, where_ref, conn_ref, conn2_ref, dims_ref, near_ref, far_ref, rows0_ref, right0_ref, right_ref, left2_ref, right2_ref, own_ref, onward_ref, psi_ref, rows_ref, rights_ref, half_ref, sum_ref, staged_ref, sems, out_sem):
    kdev, sdev, width, _ = right_ref.shape
    chips, _, tall, _ = near_ref.shape
    group = where_ref[0]
    core = where_ref[1]
    many = chips * tall
    steps = [(0, 0, rows0_ref.at[0], right0_ref, ())]
    for whose, s in ((0, 1), (1, 0), (1, 1)):
        n = len(steps) - 1
        rights = (right_ref, right2_ref)[whose]
        fetches = []
        rows = rows0_ref.at[s]
        for k in range(kdev):
            if whose == 1:
                rows = rows_ref.at[s]
                fetches.append(pltpu.make_async_copy(left2_ref.at[k, s, :, core], rows.at[k], sems.at[0, n, k]))
            fetches.append(pltpu.make_async_copy(rights.at[k, s], rights_ref.at[n, k], sems.at[1, n, k]))
        for fetch in fetches:
            fetch.start()
        steps.append((whose, s, rows, rights_ref.at[n], fetches))
    cols = lax.broadcasted_iota(jnp.int32, (tall, width), 1)
    row = lax.broadcasted_iota(jnp.int32, (tall, width), 0)

    def mask_chip(s, x, y):
        size = dims_ref[s]
        for ref, seat in ((near_ref, core), (far_ref, 1 - core)):
            start = pl.multiple_of(((x * ny + y) * 2 + seat) * tall, tall)
            kept = (cols < size) & (row + start < size)
            psi_ref[s, pl.ds(start, tall), :] = jnp.where(kept, ref[y * nx + x, s].astype(F32), 0.0).astype(BF16)

    @pl.loop(0, ny)
    def _(y):
        for x in range(nx):
            mask_chip(0, x, y)

    for s in range(1, sdev):
        for y in range(ny):
            for x in range(nx):
                mask_chip(s, x, y)

    sum_ref[...] = jnp.zeros_like(sum_ref)
    for whose, s, rows, rights, fetches in steps:
        for fetch in fetches:
            fetch.wait()
        left = rows[...].reshape(kdev * many, width)
        half_ref[...] = jnp.dot(left, psi_ref[s], preferred_element_type=F32).astype(BF16)
        for k in range(kdev):
            target = (conn_ref, conn2_ref)[whose][k, s]
            place = target % sdev + jnp.where(target // sdev != group, sdev, 0)
            sum_ref[place] += lax.dot_general(
                half_ref[k * many : (k + 1) * many, :],
                rights[k],
                (((1,), (1,)), ((), ())),
                preferred_element_type=F32,
            )
    for chip in range(chips):
        for t in range(sdev):
            staged_ref[chip, t] = sum_ref[t, chip * tall : (chip + 1) * tall, :].astype(BF16)
    leave = pltpu.make_async_copy(staged_ref, own_ref, out_sem)
    leave.start()

    @pl.loop(0, chips)
    def _(chip):
        start = pl.multiple_of(chip * tall, tall)
        for t in range(sdev):
            onward_ref[chip, t] = sum_ref[sdev + t, pl.ds(start, tall), :].astype(BF16)

    leave.wait()


def slot_sums(nx, ny, where, conn, conn2, dims, near, far, rows0, right0, right, left2, right2):
    kdev, sdev, chips, _, tall, width = left2.shape
    assert sdev == 2
    rest = 2 * sdev - 1
    block = (chips, sdev, tall, width)
    smem = pl.BlockSpec(memory_space=pltpu.SMEM)
    vmem = pl.BlockSpec(memory_space=pltpu.VMEM)
    hbm = pl.BlockSpec(memory_space=pltpu.HBM)
    many = chips * tall
    return pl.pallas_call(
        functools.partial(sums_kernel, nx, ny),
        in_specs=[smem] * 4 + [vmem] * 4 + [hbm] * 3,
        out_specs=[hbm, vmem],
        out_shape=[pltpu.HBM(block, BF16), pltpu.VMEM(block, BF16)],
        scratch_shapes=[
            pltpu.VMEM((sdev, width, width), BF16),
            pltpu.VMEM((sdev, kdev, chips, tall, width), BF16),
            pltpu.VMEM((rest, kdev, width, width), BF16),
            pltpu.VMEM((kdev * many, width), BF16),
            pltpu.VMEM((2 * sdev, many, width), F32),
            pltpu.VMEM(block, BF16),
            pltpu.SemaphoreType.DMA((2, rest, kdev)),
            pltpu.SemaphoreType.DMA,
        ],
        compiler_params=pltpu.CompilerParams(vmem_limit_bytes=24 * 2**20),
        name="slot_sums",
    )(where, conn, conn2, dims, *(in_vmem(x) for x in (near, far, rows0, right0)), *(in_hbm(x) for x in (right, left2, right2)))


def kept_entries(dims, row_start, rows, width):
    row_ids = row_start + jnp.arange(rows, dtype=jnp.int32)
    col_ids = jnp.arange(width, dtype=jnp.int32)
    return (row_ids[None, :, None] < dims[:, None, None]) & (
        col_ids[None, None, :] < dims[:, None, None]
    )


def sigma_rows(psi, left_ops, right_ops, conn, dims):
    sdev, tall, width = psi.shape
    nx, ny = lax.axis_size("x"), lax.axis_size("y")
    places = (lax.axis_index("sec"), lax.axis_index("c"), lax.axis_index(OP) * tall)
    where = jnp.stack(places).astype(jnp.int32)
    by_row = left_ops.shape[:2] + (nx * ny, 2, tall, width)
    left2 = from_partner(left_ops).reshape(by_row)
    right2 = from_partner(right_ops)
    conn2 = from_partner(conn)
    left = left_ops.reshape(by_row)
    rows0, right0 = fetched(where, left, right_ops)
    by_x = shared(psi, ("y", "x"), nx * ny)
    kept = kept_entries(dims, places[2], tall, width)
    by_x, kept = lax.optimization_barrier((by_x, kept))
    other = from_partner(by_x)
    own, onward = slot_sums(nx, ny, where, conn, conn2, dims, by_x, other, rows0, right0, right_ops, left2, right2)
    by_chip = (nx, ny, sdev, tall, width)
    onward = exchanged(onward, "x").reshape(by_chip).astype(F32).sum(axis=0).astype(BF16)
    far = around(onward)
    near = ahead(onward)
    own = exchanged(own, "x").reshape(by_chip).astype(F32).sum(axis=0)
    summed = exchanged((own + far.astype(F32) + near.astype(F32)).astype(BF16), "y").astype(F32).sum(axis=0)
    return jnp.where(kept, summed, jnp.zeros_like(summed)).astype(BF16)


def solution(mesh):
    finer = Mesh(mesh.devices.reshape(4, 4, 2, mesh.shape["sec"]), OP + ("sec",))
    in_specs = (
        P("sec", OP, None),
        P(OP, "sec", None, None),
        P(OP, "sec", None, None),
        P(OP, "sec"),
        P("sec"),
    )
    out_specs = P("sec", OP, None)
    return jax.shard_map(sigma_rows, mesh=finer, in_specs=in_specs, out_specs=out_specs, check_vma=False)
```
